128 devices in a mesh: dp: 2 (over core), ep: 64 (over x, y, z).
Axes of the slice: x: 4, y: 4, z: 4, core: 2. Of those that a mesh axis runs over, the one named last changes fastest.
Arguments:
- x: bfloat16 [2, 64, 256, 2048], P('dp', 'ep'), parts along dimension 0
- expert: int32 [2, 64, 256, 8], P('dp', 'ep'), parts along dimension 0
- slot: int32 [2, 64, 256, 8], P('dp', 'ep'), parts along dimension 0
- gate: float32 [2, 64, 256, 8], P('dp', 'ep'), parts along dimension 0
- w_gate: bfloat16 [128, 2048, 1536], P('ep')
- w_up: bfloat16 [128, 2048, 1536], P('ep')
- w_down: bfloat16 [128, 1536, 2048], P('ep')
Outputs:
- y: bfloat16 [2, 64, 256, 2048], P('dp', 'ep'), parts along dimension 0
There are 2 independent parts. The reference program is written for one: setup_inputs(seed, part) draws one part's arguments, and reference() takes and returns one part's arrays. A program takes and returns all parts, laid end to end along the dimension named above; an argument that names none is the same for every part.
All inputs are finite; a program needn't handle non-finite values.
Results may differ from the reference program's by a relative error of at most 0.009.
Values are sent between devices in bfloat16 or wider.
A program may use at most 1.5 GiB of HBM per device.

```python
import jax
import jax.numpy as jnp

MEMBERS = 64
TOKENS = 256
D = 2048
FF = 1536
TOP = 8
EXPERTS = 128
SLOTS = 5 * TOKENS * TOP // (4 * EXPERTS)


def setup_inputs(seed: int = 0, part: int = 0) -> dict:
    own, k1, k2, k3, k4, k5, k6 = jax.random.split(jax.random.key(seed), 7)
    kx, ke, kl, kg = jax.random.split(jax.random.fold_in(own, part), 4)
    devices = (1, MEMBERS)
    place = jax.random.permutation(kl, jnp.arange(EXPERTS, dtype=jnp.uint32))
    slow = ((EXPERTS + (9 * place) % EXPERTS) << ((9 * place) // EXPERTS)) // EXPERTS
    wait = (jax.random.bits(ke, (*devices, TOKENS, EXPERTS), jnp.uint32) >> 10) * slow
    expert = jnp.argsort(wait, axis=-1)[..., :TOP].astype(jnp.int32)
    chosen = jax.nn.one_hot(expert, EXPERTS, dtype=jnp.int32)
    in_line = jnp.cumsum(chosen.reshape(*devices, TOKENS * TOP, EXPERTS), axis=2) - 1
    slot = jnp.sum(in_line.reshape(chosen.shape) * chosen, axis=-1)

    def one(key, rows, columns):
        return (jax.random.normal(key, (rows, columns), jnp.float32) * rows**-0.5).astype(jnp.bfloat16)

    def weights(key, rows, columns):
        return jax.lax.map(lambda k: one(k, rows, columns), jax.random.split(key, EXPERTS))

    return {
        "x": jax.random.normal(kx, (*devices, TOKENS, D), jnp.float32).astype(jnp.bfloat16),
        "expert": expert,
        "slot": slot,
        "gate": jax.nn.softmax(jax.random.normal(kg, expert.shape, jnp.float32)),
        "w_gate": weights(k1, D, FF),
        "w_up": weights(k2, D, FF),
        "w_down": weights(k3, FF, D),
    }


def einsum(form, a, b):
    return jnp.einsum(form, a.astype(jnp.float32), b.astype(jnp.float32))


def reference(x, expert, slot, gate, w_gate, w_up, w_down):
    to_expert = jax.nn.one_hot(expert, EXPERTS, dtype=jnp.bfloat16)
    to_slot = jax.nn.one_hot(slot, SLOTS, dtype=jnp.bfloat16)
    weighted = to_expert * gate[..., None].astype(jnp.bfloat16)
    dispatch = einsum("abtke,abtkc->abtec", to_expert, to_slot).astype(jnp.bfloat16)
    combine = einsum("abtke,abtkc->abtec", weighted, to_slot).astype(jnp.bfloat16)
    z = einsum("abtec,abtd->aebcd", dispatch, x).astype(jnp.bfloat16)
    h = jax.nn.silu(einsum("aebcd,edf->aebcf", z, w_gate))
    h = (h * einsum("aebcd,edf->aebcf", z, w_up)).astype(jnp.bfloat16)
    out = einsum("aebcf,efd->aebcd", h, w_down).astype(jnp.bfloat16)
    y = einsum("abtec,aebcd->abtd", combine, out)
    return y.astype(jnp.bfloat16)
```

```python
import functools

import jax
import jax.numpy as jnp
from jax import lax
from jax.experimental import pallas as pl
from jax.experimental.pallas import tpu as pltpu
from jax.sharding import PartitionSpec as P

F32, BF16, I32 = jnp.float32, jnp.bfloat16, jnp.int32
TILE = 256
LANES = 128
VMEM_LIMIT = 60 * 2**20


def iota(shape, dim):
    return lax.broadcasted_iota(I32, shape, dim)


def dot(a, b):
    return jnp.dot(a, b, preferred_element_type=F32)


def pack_kernel(post_ref, x_ref, rows_ref):
    tokens = x_ref.shape[0]
    at = iota((TILE, tokens), 0) + pl.program_id(0) * TILE
    hit = at == post_ref[0:1, :]
    for j in range(1, post_ref.shape[0]):
        hit = hit | (at == post_ref[j : j + 1, :])
    rows = dot(jnp.where(hit, 1.0, 0.0).astype(BF16), x_ref[...])
    rows_ref[...] = rows.reshape(rows_ref.shape).astype(BF16)


def pack(post, x, rows):
    tokens, depth = x.shape
    return pl.pallas_call(
        pack_kernel,
        grid=(rows // TILE,),
        in_specs=[pl.BlockSpec(post.shape, lambda i: (0, 0)), pl.BlockSpec((tokens, depth), lambda i: (0, 0))],
        out_specs=pl.BlockSpec((TILE, depth // LANES, LANES), lambda i: (i, 0, 0)),
        out_shape=jax.ShapeDtypeStruct((rows, depth // LANES, LANES), BF16),
        cost_estimate=pl.CostEstimate(flops=2 * rows * tokens * depth, bytes_accessed=2 * rows * depth, transcendentals=0),
        name="pack",
    )(post, x)


def expert_kernel(z_ref, gate_ref, up_ref, down_ref, out_ref, rows, flat, acc, in_sem, out_sem):
    f, steps = pl.program_id(0), pl.num_programs(0)
    tiles, depth = rows.shape[0] // TILE, flat.shape[1]

    def fetch(i, r):
        return pltpu.make_async_copy(z_ref.at[r], rows.at[r], in_sem.at[i])

    def put(i, r):
        return pltpu.make_async_copy(rows.at[r], out_ref.at[r], out_sem.at[i])

    @pl.when(f == 0)
    def _():
        for i in range(tiles):
            fetch(i, pl.ds(i * TILE, TILE)).start()

    def body(i, carry):
        r = pl.ds(pl.multiple_of(i * TILE, TILE), TILE)

        @pl.when(f == 0)
        def _():
            fetch(i, r).wait()
            flat[r, :] = rows[r].reshape(TILE, depth)

        z = flat[r, :]
        h = (jax.nn.silu(dot(z, gate_ref[0])) * dot(z, up_ref[0])).astype(BF16)
        part = dot(h, down_ref[0])

        @pl.when(f == 0)
        def _():
            acc[r, :] = part

        @pl.when((f > 0) & (f < steps - 1))
        def _():
            acc[r, :] += part

        @pl.when(f == steps - 1)
        def _():
            rows[r] = (acc[r, :] + part).reshape(TILE, depth // LANES, LANES).astype(BF16)
            put(i, r).start()

        return carry

    lax.fori_loop(0, tiles, body, 0)

    @pl.when(f == steps - 1)
    def _():
        for i in range(tiles):
            put(i, pl.ds(i * TILE, TILE)).wait()


def run_expert(k, z, w_gate, w_up, w_down, width=768):
    rows, depth, inner = z.shape[0], w_gate.shape[1], w_gate.shape[2]
    return pl.pallas_call(
        expert_kernel,
        grid=(inner // width,),
        in_specs=[
            pl.BlockSpec(memory_space=pl.ANY),
            pl.BlockSpec((1, depth, width), lambda f: (k, 0, f)),
            pl.BlockSpec((1, depth, width), lambda f: (k, 0, f)),
            pl.BlockSpec((1, width, depth), lambda f: (k, f, 0)),
        ],
        out_specs=pl.BlockSpec(memory_space=pl.ANY),
        out_shape=jax.ShapeDtypeStruct(z.shape, BF16),
        scratch_shapes=[
            pltpu.VMEM(z.shape, BF16),
            pltpu.VMEM((rows, depth), BF16),
            pltpu.VMEM((rows, depth), F32),
            pltpu.SemaphoreType.DMA((rows // TILE,)),
            pltpu.SemaphoreType.DMA((rows // TILE,)),
        ],
        compiler_params=pltpu.CompilerParams(vmem_limit_bytes=VMEM_LIMIT),
        cost_estimate=pl.CostEstimate(flops=6 * rows * depth * inner, bytes_accessed=6 * depth * inner, transcendentals=0),
        name="expert",
    )(z, w_gate, w_up, w_down)


def combine_kernel(place_ref, gate_ref, rows_ref, *rest):
    before_ref, (y_ref, acc) = (rest[0], rest[1:]) if len(rest) == 3 else (None, rest)
    tokens, depth = y_ref.shape
    i = pl.program_id(0)

    @pl.when(i == 0)
    def _():
        acc[...] = jnp.zeros_like(acc) if before_ref is None else before_ref[...]

    at = iota((tokens, TILE), 1) + i * TILE
    weight = jnp.zeros((tokens, TILE), F32)
    for j in range(place_ref.shape[1]):
        gate = gate_ref[:, j : j + 1].astype(BF16).astype(F32)
        weight = jnp.where(at == place_ref[:, j : j + 1], gate, weight)
    acc[...] += dot(weight.astype(BF16), rows_ref[...].reshape(TILE, depth))

    @pl.when(i == pl.num_programs(0) - 1)
    def _():
        y_ref[...] = acc[...].astype(y_ref.dtype)


def combine(place, gate, rows, before, dtype):
    tokens, depth = gate.shape[0], rows.shape[1] * rows.shape[2]
    whole = lambda a: pl.BlockSpec(a.shape, lambda i: (0, 0))
    extra = [] if before is None else [before]
    return pl.pallas_call(
        combine_kernel,
        grid=(rows.shape[0] // TILE,),
        in_specs=[whole(place), whole(gate), pl.BlockSpec((TILE, *rows.shape[1:]), lambda i: (i, 0, 0))]
        + [whole(a) for a in extra],
        out_specs=pl.BlockSpec((tokens, depth), lambda i: (0, 0)),
        scratch_shapes=[pltpu.VMEM((tokens, depth), F32)],
        out_shape=jax.ShapeDtypeStruct((tokens, depth), dtype),
        cost_estimate=pl.CostEstimate(
            flops=2 * rows.shape[0] * tokens * depth, bytes_accessed=2 * rows.shape[0] * depth, transcendentals=0
        ),
        name="combine",
    )(place, gate, rows, *extra)


def solution(mesh):
    members = mesh.shape["ep"]

    def exchange(rows):
        return lax.all_to_all(rows.reshape(members, -1, *rows.shape[1:]), "ep", 0, 0).reshape(rows.shape)

    def step(x, expert, slot, gate, w_gate, w_up, w_down):
        tokens, depth = x.shape[2:]
        slots = 5 * tokens * expert.shape[3] // (4 * 2 * members)
        x, expert, slot, gate = x[0, 0], expert[0, 0], slot[0, 0], gate[0, 0]
        row = jnp.where(slot < slots, expert // 2 * slots + slot, -1)
        place = [jnp.where(expert % 2 == k, row, -1) for k in (0, 1)]

        out = []
        for k in (0, 1):
            z = exchange(pack(place[k].T, x, members * slots))
            out.append(exchange(run_expert(k, z, w_gate, w_up, w_down)))
        first = combine(place[0], gate, out[0], None, F32)
        return combine(place[1], gate, out[1], first, BF16)[None, None]

    spread, held = P("dp", "ep"), P("ep")
    return jax.shard_map(
        step,
        mesh=mesh,
        in_specs=(spread, spread, spread, spread, held, held, held),
        out_specs=spread,
        check_vma=False,
    )
```

```python
import functools

import jax
import jax.numpy as jnp
from jax import lax
from jax.experimental import pallas as pl
from jax.experimental.pallas import tpu as pltpu
from jax.sharding import PartitionSpec as P

F32, BF16, I32 = jnp.float32, jnp.bfloat16, jnp.int32
MESH = pl.DeviceIdType.MESH
SIDE = 4
STRIDE = (SIDE * SIDE, SIDE, 1)
AXES = ((0, 1, 2), (1, 2, 0), (2, 0, 1))
GROUP = 4
WIDTH = 512
PARTS, OTHERS = range(3), range(1, SIDE)


def iota(shape, dim):
    return lax.broadcasted_iota(I32, shape, dim)


def dot(a, b):
    return jnp.dot(a, b, preferred_element_type=F32)


def kernel(slots, cols, width, meta_ref, x_ref, gate_hbm, up_hbm, down_hbm, y_ref, *rest):
    relay, back, home = rest[0:3], rest[3:6], rest[6:9]
    spread, boxes, rows, sums = rest[9:12], rest[12:15], rest[15:18], rest[18:21]
    metas, flat, acc, gate_w, up_w, down_w = rest[21:27]
    (bell_s, bell_r, tok_s, tok_r, two_s, two_r, three_s, three_r) = rest[27:35]
    (b3_s, b3_r, b2_s, b2_r, end_s, end_r, own, w_sem) = rest[35:43]

    tokens, depth = x_ref.shape
    top = meta_ref.shape[0] // 2
    inner = gate_hbm.shape[2]
    steps = inner // width
    plane = SIDE * SIDE * slots
    offset = [sum(cols[:c]) for c in PARTS]
    me, dp = lax.axis_index("ep"), lax.axis_index("dp")
    at = (me // STRIDE[0], lax.rem(me // STRIDE[1], SIDE), lax.rem(me, SIDE))

    def other(axis, d):
        return lax.rem(at[axis] + d, SIDE)

    def remote(src, dst, send, recv, axis, d):
        target = me + (other(axis, d) - at[axis]) * STRIDE[axis]
        return pltpu.make_async_remote_copy(
            src_ref=src, dst_ref=dst, send_sem=send, recv_sem=recv, device_id=(dp, target), device_id_type=MESH
        )


    def third(ref, c, p):
        return (ref.at[:, :, p], ref.at[p], ref.at[:, p])[c]

    def second(ref, c, p):
        return ref.at[p] if c == 2 else ref.at[:, p]


    def bell(c, d):
        return remote(meta_ref, metas.at[c, at[AXES[c][0]]], bell_s.at[c, d - 1], bell_r.at[c, d - 1], AXES[c][0], d)

    def token(c, d):
        src = x_ref.at[:, pl.ds(offset[c], cols[c])]
        return remote(src, spread[c].at[at[AXES[c][0]]], tok_s.at[c, d - 1], tok_r.at[c, d - 1], AXES[c][0], d)

    def two(k, c, d):
        axis = AXES[c][1]
        src, dst = boxes[c].at[other(axis, d)], second(relay[c].at[k], c, at[axis])
        return remote(src, dst, two_s.at[k, c, d - 1], two_r.at[k, c, d - 1], axis, d)

    def two_own(k, c):
        p = at[AXES[c][1]]
        return pltpu.make_async_copy(boxes[c].at[p], second(relay[c].at[k], c, p), own.at[0, k, c])

    def three(k, c, d):
        axis = AXES[c][2]
        src, dst = relay[c].at[k, :, :, other(axis, d)], third(rows[c].at[k], c, at[axis])
        return remote(src, dst, three_s.at[k, c, d - 1], three_r.at[k, c, d - 1], axis, d)

    def three_own(k, c):
        p = at[AXES[c][2]]
        return pltpu.make_async_copy(relay[c].at[k, :, :, p], third(rows[c].at[k], c, p), own.at[1, k, c])

    def back_three(k, c, d):
        axis = AXES[c][2]
        src, dst = third(rows[c].at[k], c, other(axis, d)), back[c].at[k, at[axis]]
        return remote(src, dst, b3_s.at[k, c, d - 1], b3_r.at[k, c, d - 1], axis, d)

    def back_three_own(k, c):
        p = at[AXES[c][2]]
        return pltpu.make_async_copy(third(rows[c].at[k], c, p), back[c].at[k, p], own.at[2, k, c])

    def returned(k, c, p):
        return back[c].at[k, :, p] if c == 2 else back[c].at[k, :, :, p]

    def back_two(k, c, d):
        axis = AXES[c][1]
        src, dst = returned(k, c, other(axis, d)), home[c].at[k, at[axis]]
        return remote(src, dst, b2_s.at[k, c, d - 1], b2_r.at[k, c, d - 1], axis, d)

    def load_home(k, c, d):
        p = other(AXES[c][1], SIDE - d)
        src = returned(k, c, p) if d == 0 else home[c].at[k, p]
        return pltpu.make_async_copy(src, boxes[c].at[p], own.at[3 + d, k, c])

    def end(c, d):
        axis = AXES[c][0]
        src, dst = spread[c].at[other(axis, d)], sums[c].at[at[axis]]
        return remote(src, dst, end_s.at[c, d - 1], end_r.at[c, d - 1], axis, d)

    def weights(n):
        k, cut, s = n // steps, pl.ds(lax.rem(n, steps) * width, width), lax.rem(n, 2)
        return (
            pltpu.make_async_copy(gate_hbm.at[k, :, cut], gate_w.at[s], w_sem.at[s, 0]),
            pltpu.make_async_copy(up_hbm.at[k, :, cut], up_w.at[s], w_sem.at[s, 1]),
            pltpu.make_async_copy(down_hbm.at[k, cut, :], down_w.at[s], w_sem.at[s, 2]),
        )


    def place_of_row(k, c):
        r = iota((plane, tokens), 0)
        a1, a2, a3 = AXES[c]
        device = at[a1] * STRIDE[a1] + r // (SIDE * slots) * STRIDE[a2] + r // slots % SIDE * STRIDE[a3]
        return ((2 * device + k) * slots + r % slots).astype(F32)

    def pack(k, c):
        place = place_of_row(k, c)

        def one(s, carry):
            hit = place == metas[c, s, 0:1, :]
            for j in range(1, top):
                hit = hit | (place == metas[c, s, j : j + 1, :])
            out = dot(jnp.where(hit, 1.0, 0.0).astype(BF16), spread[c][s]).astype(BF16)
            boxes[c][:, s] = out.reshape(SIDE, SIDE, slots // GROUP, GROUP, cols[c])
            return carry

        lax.fori_loop(0, SIDE, one, 0)

    def combine(k, c):
        place = place_of_row(k, c)
        span = pl.ds(offset[c], cols[c])

        def one(s, carry):
            weight = jnp.zeros((plane, tokens), F32)
            for j in range(top):
                gate = metas[c, s, top + j : top + j + 1, :].astype(BF16).astype(F32)
                weight = jnp.where(place == metas[c, s, j : j + 1, :], gate, weight)
            got = boxes[c][:, :, s].reshape(plane, cols[c])
            part = lax.dot_general(
                weight.astype(BF16), got, (((0,), (0,)), ((), ())), preferred_element_type=F32
            )
            r = pl.ds(pl.multiple_of(s * tokens, tokens), tokens)
            if k == 0:
                acc[r, span] = part
            else:
                acc[r, span] += part
                spread[c][s] = acc[r, span].astype(BF16)
            return carry

        lax.fori_loop(0, SIDE, one, 0)

    def expert(k, between):
        tile = plane

        def step(f):
            n = k * steps + f
            s = lax.rem(n, 2)
            if n + 1 < 2 * steps:
                for copy in weights(n + 1):
                    copy.start()
            for copy in weights(n):
                copy.wait()

            def body(i, carry):
                r = pl.ds(pl.multiple_of(i * tile, tile), tile)
                if f == 0:
                    for c in PARTS:
                        flat[r, pl.ds(offset[c], cols[c])] = rows[c][k, i].reshape(tile, cols[c])
                z = flat[r, :]
                h = (jax.nn.silu(dot(z, gate_w[s])) * dot(z, up_w[s])).astype(BF16)
                part = dot(h, down_w[s])
                if f == 0:
                    acc[r, :] = part
                elif f < steps - 1:
                    acc[r, :] += part
                else:
                    flat[r, :] = (acc[r, :] + part).astype(BF16)
                    for c in PARTS:
                        out = flat[r, pl.ds(offset[c], cols[c])]
                        rows[c][k, i] = out.reshape(SIDE, SIDE, slots // GROUP, GROUP, cols[c])
                return carry

            lax.fori_loop(0, SIDE, body, 0)

        for f in range(steps):
            step(f)
            between(f)


    barrier = pltpu.get_barrier_semaphore()
    for axis in range(3):
        for d in OTHERS:
            target = me + (other(axis, d) - at[axis]) * STRIDE[axis]
            pl.semaphore_signal(barrier, inc=1, device_id=(dp, target), device_id_type=MESH)
    for copy in weights(0):
        copy.start()
    for c in PARTS:
        metas[c, at[AXES[c][0]]] = meta_ref[...]
        spread[c][at[AXES[c][0]]] = x_ref[:, pl.ds(offset[c], cols[c])]
    pl.semaphore_wait(barrier, 3 * (SIDE - 1))

    for c in PARTS:
        for d in OTHERS:
            bell(c, d).start()
            token(c, d).start()

    def relay_two(k, c):
        two_own(k, c).wait()
        for d in OTHERS:
            two(k, c, d).wait()
        for d in OTHERS:
            three(k, c, d).start()
        three_own(k, c).start()

    def send_boxes(k, c):
        pack(k, c)
        for d in OTHERS:
            two(k, c, d).start()
        two_own(k, c).start()

    for c in PARTS:
        for d in OTHERS:
            bell(c, d).wait()
            token(c, d).wait()
        send_boxes(0, c)
    for c in PARTS:
        relay_two(0, c)
        send_boxes(1, c)

    def wait_rows(k):
        for c in PARTS:
            for d in OTHERS:
                three(k, c, d).wait()
            three_own(k, c).wait()

    def send_back(k):
        for c in PARTS:
            for d in OTHERS:
                back_three(k, c, d).start()
            back_three_own(k, c).start()

    def relay_back(k, c):
        back_three_own(k, c).wait()
        for d in OTHERS:
            back_three(k, c, d).wait()
        for d in OTHERS:
            back_two(k, c, d).start()

    def bring_home(k, c):
        load_home(k, c, 0).start()
        for d in OTHERS:
            back_two(k, c, d).wait()
            load_home(k, c, d).start()
        for d in range(SIDE):
            load_home(k, c, d).wait()
        combine(k, c)

    def during_first(f):
        if f == 0:
            for c in PARTS:
                relay_two(1, c)

    def during_second(f):
        if f == steps - 2:
            for c in PARTS:
                relay_back(0, c)

    wait_rows(0)
    expert(0, during_first)
    send_back(0)
    wait_rows(1)
    expert(1, during_second)
    send_back(1)
    for c in PARTS:
        bring_home(0, c)
    for c in PARTS:
        relay_back(1, c)
    for c in PARTS:
        bring_home(1, c)
        for d in OTHERS:
            end(c, d).start()
    for c in PARTS:
        span = pl.ds(offset[c], cols[c])
        axis = AXES[c][0]
        total = acc[pl.ds(pl.multiple_of(at[axis] * tokens, tokens), tokens), span]
        for d in OTHERS:
            end(c, d).wait()
        for d in OTHERS:
            total += sums[c][other(axis, d)].astype(F32)
        y_ref[:, span] = total.astype(y_ref.dtype)


def moe(meta, x, w_gate, w_up, w_down, slots):
    (tokens, depth), inner = x.shape, w_gate.shape[2]
    third = depth // 128 // 3 * 128
    cols = (third, third, depth - 2 * third)
    width = min(WIDTH, inner // 2)
    plane = SIDE * SIDE * slots
    box = lambda c, *lead: (*lead, SIDE, SIDE, SIDE, slots // GROUP, GROUP, cols[c])
    hbm = [jax.ShapeDtypeStruct(box(c, 2), BF16) for _ in range(3) for c in PARTS]
    dma = pltpu.SemaphoreType.DMA
    n = SIDE - 1
    out = pl.pallas_call(
        functools.partial(kernel, slots, cols, width),
        in_specs=[pl.BlockSpec(memory_space=pltpu.VMEM)] * 2 + [pl.BlockSpec(memory_space=pl.ANY)] * 3,
        out_specs=[pl.BlockSpec(memory_space=pltpu.VMEM)] + [pl.BlockSpec(memory_space=pl.ANY)] * len(hbm),
        out_shape=[jax.ShapeDtypeStruct((tokens, depth), BF16)] + hbm,
        scratch_shapes=[pltpu.VMEM((SIDE, tokens, cols[c]), BF16) for c in PARTS]
        + [pltpu.VMEM(box(c), BF16) for c in PARTS]
        + [pltpu.VMEM(box(c, 2), BF16) for c in PARTS]
        + [pltpu.VMEM((SIDE, tokens, cols[c]), BF16) for c in PARTS]
        + [
            pltpu.VMEM((3, SIDE, *meta.shape), F32),
            pltpu.VMEM((SIDE * plane, depth), BF16),
            pltpu.VMEM((SIDE * plane, depth), F32),
            pltpu.VMEM((2, depth, width), BF16),
            pltpu.VMEM((2, depth, width), BF16),
            pltpu.VMEM((2, width, depth), BF16),
        ]
        + [dma((3, n))] * 4
        + [dma((2, 3, n))] * 8
        + [dma((3, n))] * 2
        + [dma((3 + SIDE, 2, 3)), dma((2, 3))],
        compiler_params=pltpu.CompilerParams(
            collective_id=0, has_side_effects=True, vmem_limit_bytes=67043328
        ),
        name="moe",
    )(meta, x, w_gate, w_up, w_down)
    return out[0]


def solution(mesh):
    members = mesh.shape["ep"]

    def step(x, expert, slot, gate, w_gate, w_up, w_down):
        tokens = x.shape[2]
        slots = 5 * tokens * expert.shape[3] // (4 * 2 * members)
        x, expert, slot, gate = x[0, 0], expert[0, 0], slot[0, 0], gate[0, 0]
        place = jnp.where(slot < slots, expert * slots + slot, -1)
        meta = jnp.concatenate([place.astype(F32).T, gate.T])
        return moe(meta, x, w_gate, w_up, w_down, slots)[None, None]

    spread, held = P("dp", "ep"), P("ep")
    return jax.shard_map(
        step,
        mesh=mesh,
        in_specs=(spread, spread, spread, spread, held, held, held),
        out_specs=spread,
        check_vma=False,
    )
```

```python
import contextlib
import functools

import jax
import jax.numpy as jnp
from jax import lax
from jax.experimental import pallas as pl
from jax.experimental.pallas import tpu as pltpu
from jax.sharding import PartitionSpec as P

F32, BF16, I32 = jnp.float32, jnp.bfloat16, jnp.int32
MESH = pl.DeviceIdType.MESH
SIDE = 4
STRIDE = (SIDE * SIDE, SIDE, 1)
AXES = ((0, 1, 2), (1, 2, 0), (2, 0, 1)) * 2
GROUP = 4
WIDTH = 512
PARTS, ORDERS, OTHERS = range(6), range(3), range(1, SIDE)
FIRST, SECOND = (4, 4, 5, 5, 6, 7), (2, 3, 4, 5, 6, 7)


def phase(name):
    return contextlib.nullcontext()


def iota(shape, dim):
    return lax.broadcasted_iota(I32, shape, dim)


def dot(a, b):
    return jnp.dot(a, b, preferred_element_type=F32)


def kernel(slots, cols, width, meta_ref, x_ref, gate_hbm, up_hbm, down_hbm, y_ref, *rest):
    rest = list(rest)
    take = lambda n: [rest.pop(0) for _ in range(n)]
    relay, back, home, spread, boxes, rows, sums = (take(len(PARTS)) for _ in range(7))
    metas, mask, flat, acc, gate_w, up_w, down_w = take(7)
    bell_s, bell_r, tok_s, tok_r, two_s, two_r, three_s, three_r = take(8)
    b3_s, b3_r, b2_s, b2_r, end_s, end_r, own, w_sem = take(8)

    tokens, depth = x_ref.shape
    top = meta_ref.shape[0] // 2
    inner = gate_hbm.shape[2]
    steps = inner // width
    plane = SIDE * SIDE * slots
    offset = [sum(cols[:c]) for c in PARTS]
    me, dp = lax.axis_index("ep"), lax.axis_index("dp")
    turn = lax.rem(dp, 2)
    chip = (me // STRIDE[0], lax.rem(me // STRIDE[1], SIDE), lax.rem(me, SIDE))
    turned = lambda v: tuple(v[i] + turn * (v[(i + 1) % 3] - v[i]) for i in range(3))
    at, stride = turned(chip), turned(STRIDE)

    def other(axis, d):
        return lax.rem(at[axis] + d, SIDE)

    def remote(src, dst, send, recv, axis, d):
        target = me + (other(axis, d) - at[axis]) * stride[axis]
        return pltpu.make_async_remote_copy(
            src_ref=src, dst_ref=dst, send_sem=send, recv_sem=recv, device_id=(dp, target), device_id_type=MESH
        )


    def third(ref, c, p):
        return (ref.at[:, :, p], ref.at[p], ref.at[:, p])[c % 3]

    def second(ref, c, p):
        return ref.at[p] if c % 3 == 2 else ref.at[:, p]


    def bell(c, d):
        return remote(meta_ref, metas.at[c, at[AXES[c][0]]], bell_s.at[c, d - 1], bell_r.at[c, d - 1], AXES[c][0], d)

    def token(c, d):
        src = x_ref.at[:, pl.ds(offset[c], cols[c])]
        return remote(src, spread[c].at[at[AXES[c][0]]], tok_s.at[c, d - 1], tok_r.at[c, d - 1], AXES[c][0], d)

    def two(k, c, d):
        axis = AXES[c][1]
        src, dst = boxes[c].at[other(axis, d)], second(relay[c].at[k], c, at[axis])
        return remote(src, dst, two_s.at[k, c, d - 1], two_r.at[k, c, d - 1], axis, d)

    def two_own(k, c):
        p = at[AXES[c][1]]
        return pltpu.make_async_copy(boxes[c].at[p], second(relay[c].at[k], c, p), own.at[0, k, c])

    def three(k, c, d):
        axis = AXES[c][2]
        src, dst = relay[c].at[k, :, :, other(axis, d)], third(rows[c].at[k], c, at[axis])
        return remote(src, dst, three_s.at[k, c, d - 1], three_r.at[k, c, d - 1], axis, d)

    def three_own(k, c):
        p = at[AXES[c][2]]
        return pltpu.make_async_copy(relay[c].at[k, :, :, p], third(rows[c].at[k], c, p), own.at[1, k, c])

    def back_three(k, c, d):
        axis = AXES[c][2]
        src, dst = third(rows[c].at[k], c, other(axis, d)), back[c].at[k, at[axis]]
        return remote(src, dst, b3_s.at[k, c, d - 1], b3_r.at[k, c, d - 1], axis, d)

    def back_three_own(k, c):
        p = at[AXES[c][2]]
        return pltpu.make_async_copy(third(rows[c].at[k], c, p), back[c].at[k, p], own.at[2, k, c])

    def returned(k, c, p):
        return back[c].at[k, :, p] if c % 3 == 2 else back[c].at[k, :, :, p]

    def back_two(k, c, d):
        axis = AXES[c][1]
        src, dst = returned(k, c, other(axis, d)), home[c].at[k, at[axis]]
        return remote(src, dst, b2_s.at[k, c, d - 1], b2_r.at[k, c, d - 1], axis, d)

    def load_home(k, c, d):
        p = other(AXES[c][1], SIDE - d)
        src = returned(k, c, p) if d == 0 else home[c].at[k, p]
        return pltpu.make_async_copy(src, boxes[c].at[p], own.at[3 + d, k, c])

    def end(c, d):
        axis = AXES[c][0]
        src, dst = spread[c].at[other(axis, d)], sums[c].at[at[axis]]
        return remote(src, dst, end_s.at[c, d - 1], end_r.at[c, d - 1], axis, d)

    def weights(n):
        k, cut, s = n // steps, pl.ds(lax.rem(n, steps) * width, width), lax.rem(n, 2)
        return (
            pltpu.make_async_copy(gate_hbm.at[k, :, cut], gate_w.at[s], w_sem.at[s, 0]),
            pltpu.make_async_copy(up_hbm.at[k, :, cut], up_w.at[s], w_sem.at[s, 1]),
            pltpu.make_async_copy(down_hbm.at[k, cut, :], down_w.at[s], w_sem.at[s, 2]),
        )


    def place_of_row(k, c):
        r = iota((plane, tokens), 0)
        a1, a2, a3 = AXES[c]
        device = at[a1] * stride[a1] + r // (SIDE * slots) * stride[a2] + r // slots % SIDE * stride[a3]
        return ((2 * device + k) * slots + r % slots).astype(F32)

    def choose(k, c):
        place = place_of_row(k, c)

        def one(s, carry):
            hit = place == metas[c, s, 0:1, :]
            for j in range(1, top):
                hit = hit | (place == metas[c, s, j : j + 1, :])
            mask[c, s] = jnp.where(hit, 1.0, 0.0).astype(BF16)
            return carry

        lax.fori_loop(0, SIDE, one, 0)

    def weigh(k, c):
        place = place_of_row(k, c)

        def one(s, carry):
            weight = jnp.zeros((plane, tokens), F32)
            for j in range(top):
                gate = metas[c, s, top + j : top + j + 1, :].astype(BF16).astype(F32)
                weight = jnp.where(place == metas[c, s, j : j + 1, :], gate, weight)
            mask[c, s] = weight.astype(BF16)
            return carry

        lax.fori_loop(0, SIDE, one, 0)

    def pack(c):
        def one(s, carry):
            out = dot(mask[c % 3, s], spread[c][s]).astype(BF16)
            boxes[c][:, s] = out.reshape(SIDE, SIDE, slots // GROUP, GROUP, cols[c])
            return carry

        lax.fori_loop(0, SIDE, one, 0)

    def combine(k, c):
        span = pl.ds(offset[c], cols[c])

        def one(s, carry):
            got = boxes[c][:, :, s].reshape(plane, cols[c])
            part = lax.dot_general(mask[c % 3, s], got, (((0,), (0,)), ((), ())), preferred_element_type=F32)
            r = pl.ds(pl.multiple_of(s * tokens, tokens), tokens)
            if k == 0:
                acc[r, span] = part
            else:
                part += acc[r, span]
                acc[r, span] = part
                spread[c][s] = part.astype(BF16)
            return carry

        lax.fori_loop(0, SIDE, one, 0)

    def expert(k, errands):
        tile = plane

        def step(f):
            n = k * steps + f
            s = lax.rem(n, 2)
            if n + 1 < 2 * steps:
                for copy in weights(n + 1):
                    copy.start()
            for copy in weights(n):
                copy.wait()

            def body(i, carry):
                r = pl.ds(pl.multiple_of(i * tile, tile), tile)
                if f == 0:
                    for c in PARTS:
                        flat[r, pl.ds(offset[c], cols[c])] = rows[c][k, i].reshape(tile, cols[c])
                z = flat[r, :]
                h = (jax.nn.silu(dot(z, gate_w[s])) * dot(z, up_w[s])).astype(BF16)
                part = dot(h, down_w[s])
                if f == 0:
                    acc[r, :] = part
                elif f < steps - 1:
                    acc[r, :] += part
                else:
                    flat[r, :] = (acc[r, :] + part).astype(BF16)
                    for c in PARTS:
                        out = flat[r, pl.ds(offset[c], cols[c])]
                        rows[c][k, i] = out.reshape(SIDE, SIDE, slots // GROUP, GROUP, cols[c])
                for when, errand in errands:
                    if when // SIDE == f:
                        pl.when(i == when % SIDE)(errand)
                return carry

            lax.fori_loop(0, SIDE, body, 0)

        for f in range(steps):
            with phase(f"expert_{k}{f}"):
                step(f)


    barrier = pltpu.get_barrier_semaphore()
    for axis in range(3):
        for d in OTHERS:
            target = me + (other(axis, d) - at[axis]) * stride[axis]
            pl.semaphore_signal(barrier, inc=1, device_id=(dp, target), device_id_type=MESH)
    for copy in weights(0):
        copy.start()
    for c in ORDERS:
        metas[c, at[AXES[c][0]]] = meta_ref[...]
    for c in PARTS:
        spread[c][at[AXES[c][0]]] = x_ref[:, pl.ds(offset[c], cols[c])]
    with phase("barrier"):
        pl.semaphore_wait(barrier, 3 * (SIDE - 1))

    for d in OTHERS:
        for c in ORDERS:
            bell(c, d).start()
    for c in PARTS:
        for d in OTHERS:
            token(c, d).start()

    def relay_two(k, c):
        two_own(k, c).wait()
        for d in OTHERS:
            two(k, c, d).wait()
        for d in OTHERS:
            three(k, c, d).start()
        three_own(k, c).start()

    def send_boxes(k, c):
        pack(c)
        for d in OTHERS:
            two(k, c, d).start()
        two_own(k, c).start()

    for c in ORDERS:
        with phase(f"choose_0{c}"):
            for d in OTHERS:
                bell(c, d).wait()
            choose(0, c)
    for c in PARTS:
        with phase(f"spread_wait_{c}"):
            for d in OTHERS:
                token(c, d).wait()
        with phase(f"pack_0{c}"):
            send_boxes(0, c)
    with phase("choose_1"):
        for c in ORDERS:
            choose(1, c)
    for c in PARTS:
        with phase(f"relay_two_0{c}"):
            relay_two(0, c)
    for c in PARTS:
        with phase(f"pack_1{c}"):
            send_boxes(1, c)
    with phase("weigh_0"):
        for c in ORDERS:
            weigh(0, c)

    def wait_rows(k):
        for c in PARTS:
            for d in OTHERS:
                three(k, c, d).wait()
            three_own(k, c).wait()

    def send_back(k):
        for c in PARTS:
            for d in OTHERS:
                back_three(k, c, d).start()
            back_three_own(k, c).start()

    def relay_back(k, c):
        back_three_own(k, c).wait()
        for d in OTHERS:
            back_three(k, c, d).wait()
        for d in OTHERS:
            back_two(k, c, d).start()

    def bring_home(k, c):
        with phase(f"home_{k}{c}"):
            load_home(k, c, 0).start()
            for d in OTHERS:
                back_two(k, c, d).wait()
                load_home(k, c, d).start()
        with phase(f"load_{k}{c}"):
            for d in range(SIDE):
                load_home(k, c, d).wait()
        with phase(f"combine_{k}{c}"):
            combine(k, c)

    def errands(act, whens):
        out = []
        for c, when in zip(PARTS, whens):

            def errand(c=c):
                with phase(f"{act.__name__}_{c}"):
                    act(c)

            out.append((when, errand))
        return out

    def forward(c):
        relay_two(1, c)

    def forward_back(c):
        relay_back(0, c)

    with phase("wait_rows_0"):
        wait_rows(0)
    expert(0, errands(forward, FIRST))
    send_back(0)
    with phase("wait_rows_1"):
        wait_rows(1)
    expert(1, errands(forward_back, SECOND))
    send_back(1)
    for c in PARTS:
        bring_home(0, c)
    with phase("weigh_1"):
        for c in ORDERS:
            weigh(1, c)
    for c in PARTS:
        with phase(f"relay_back_1{c}"):
            relay_back(1, c)
    for c in PARTS:
        bring_home(1, c)
        for d in OTHERS:
            end(c, d).start()
    for c in PARTS:
        span = pl.ds(offset[c], cols[c])
        axis = AXES[c][0]
        total = acc[pl.ds(pl.multiple_of(at[axis] * tokens, tokens), tokens), span]
        with phase(f"end_{c}"):
            for d in OTHERS:
                end(c, d).wait()
        for d in OTHERS:
            total += sums[c][other(axis, d)].astype(F32)
        y_ref[:, span] = total.astype(y_ref.dtype)


def moe(meta, x, w_gate, w_up, w_down, slots):
    (tokens, depth), inner = x.shape, w_gate.shape[2]
    lanes, more = divmod(depth // 128, len(PARTS))
    cols = tuple(128 * (lanes + (c in (0, 1, 4, 5, 2, 3)[:more])) for c in PARTS)
    width = min(WIDTH, inner // 2)
    plane = SIDE * SIDE * slots
    box = lambda c, *lead: (*lead, SIDE, SIDE, SIDE, slots // GROUP, GROUP, cols[c])
    hbm = [jax.ShapeDtypeStruct(box(c, 2), BF16) for _ in range(3) for c in PARTS]
    dma = pltpu.SemaphoreType.DMA
    n, p = SIDE - 1, len(PARTS)
    out = pl.pallas_call(
        functools.partial(kernel, slots, cols, width),
        in_specs=[pl.BlockSpec(memory_space=pltpu.VMEM)] * 2 + [pl.BlockSpec(memory_space=pl.ANY)] * 3,
        out_specs=[pl.BlockSpec(memory_space=pltpu.VMEM)] + [pl.BlockSpec(memory_space=pl.ANY)] * len(hbm),
        out_shape=[jax.ShapeDtypeStruct((tokens, depth), BF16)] + hbm,
        scratch_shapes=[pltpu.VMEM((SIDE, tokens, cols[c]), BF16) for c in PARTS]
        + [pltpu.VMEM(box(c), BF16) for c in PARTS]
        + [pltpu.VMEM(box(c, 2), BF16) for c in PARTS]
        + [pltpu.VMEM((SIDE, tokens, cols[c]), BF16) for c in PARTS]
        + [
            pltpu.VMEM((3, SIDE, *meta.shape), F32),
            pltpu.VMEM((3, SIDE, plane, tokens), BF16),
            pltpu.VMEM((SIDE * plane, depth), BF16),
            pltpu.VMEM((SIDE * plane, depth), F32),
            pltpu.VMEM((2, depth, width), BF16),
            pltpu.VMEM((2, depth, width), BF16),
            pltpu.VMEM((2, width, depth), BF16),
        ]
        + [dma((3, n))] * 2
        + [dma((p, n))] * 2
        + [dma((2, p, n))] * 8
        + [dma((p, n))] * 2
        + [dma((3 + SIDE, 2, p)), dma((2, 3))],
        compiler_params=pltpu.CompilerParams(
            collective_id=0, has_side_effects=True, vmem_limit_bytes=67043328
        ),
        name="moe",
    )(meta, x, w_gate, w_up, w_down)
    return out[0]


def solution(mesh):
    members = mesh.shape["ep"]

    def step(x, expert, slot, gate, w_gate, w_up, w_down):
        tokens = x.shape[2]
        slots = 5 * tokens * expert.shape[3] // (4 * 2 * members)
        x, expert, slot, gate = x[0, 0], expert[0, 0], slot[0, 0], gate[0, 0]
        place = jnp.where(slot < slots, expert * slots + slot, -1)
        meta = jnp.concatenate([place.astype(F32).T, gate.T])
        return moe(meta, x, w_gate, w_up, w_down, slots)[None, None]

    spread, held = P("dp", "ep"), P("ep")
    return jax.shard_map(
        step,
        mesh=mesh,
        in_specs=(spread, spread, spread, spread, held, held, held),
        out_specs=spread,
        check_vma=False,
    )
```

```python
import contextlib
import functools

import jax
import jax.numpy as jnp
from jax import lax
from jax.experimental import pallas as pl
from jax.experimental.pallas import tpu as pltpu
from jax.sharding import PartitionSpec as P

F32, BF16, I32 = jnp.float32, jnp.bfloat16, jnp.int32
MESH = pl.DeviceIdType.MESH
SIDE = 4
STRIDE = (SIDE * SIDE, SIDE, 1)
AXES = ((0, 1, 2), (1, 2, 0), (2, 0, 1)) * 2
GROUP = 4
WIDTH = 512
PARTS, ORDERS, OTHERS = range(6), range(3), range(1, SIDE)
FIRST, SECOND = (2, 2, 3, 5, 5, 6), (2, 3, 4, 5, 7, 7)
WIDE = (0, 1, 2, 4, 3, 5)


def phase(name):
    return contextlib.nullcontext()


def iota(shape, dim):
    return lax.broadcasted_iota(I32, shape, dim)


def dot(a, b):
    return jnp.dot(a, b, preferred_element_type=F32)


def kernel(slots, cols, width, expert_hbm, slot_hbm, score_hbm, x_hbm, gate_hbm, up_hbm, down_hbm, y_hbm, *rest):
    rest = list(rest)
    take = lambda n: [rest.pop(0) for _ in range(n)]
    relay, back, home, spread, boxes, rows, sums = (take(len(PARTS)) for _ in range(7))
    expert_v, slot_v, score_v, meta, metas, mask, flat, acc, gate_w, up_w, down_w = take(11)
    bell_s, bell_r, tok_s, tok_r, pass_s, pass_r, two_s, two_r, three_s, three_r = take(10)
    b3_s, b3_r, b2_s, b2_r, end_s, end_r, own, w_sem, x_sem, arg_sem = take(10)
    y_v, y_sem = take(2)

    tokens, depth = x_hbm.shape
    top = expert_v.shape[0]
    inner = gate_hbm.shape[2]
    steps = inner // width
    plane = SIDE * SIDE * slots
    offset = [sum(cols[:c]) for c in PARTS]
    me, dp = lax.axis_index("ep"), lax.axis_index("dp")
    turn = lax.rem(dp, 2)
    chip = (me // STRIDE[0], lax.rem(me // STRIDE[1], SIDE), lax.rem(me, SIDE))
    turned = lambda v: tuple(v[i] + turn * (v[(i + 1) % 3] - v[i]) for i in range(3))
    at, stride = turned(chip), turned(STRIDE)

    def other(axis, d):
        return lax.rem(at[axis] + d, SIDE)

    def remote(src, dst, send, recv, axis, d):
        target = me + (other(axis, d) - at[axis]) * stride[axis]
        return pltpu.make_async_remote_copy(
            src_ref=src, dst_ref=dst, send_sem=send, recv_sem=recv, device_id=(dp, target), device_id_type=MESH
        )


    def third(ref, c, p):
        return (ref.at[:, :, p], ref.at[p], ref.at[:, p])[c % 3]

    def second(ref, c, p):
        return ref.at[p] if c % 3 == 2 else ref.at[:, p]


    def bell(c, d):
        return remote(meta, metas.at[c, at[AXES[c][0]]], bell_s.at[c], bell_r.at[c], AXES[c][0], d)

    def token_own(c):
        return pltpu.make_async_copy(
            x_hbm.at[:, pl.ds(offset[c], cols[c])], spread[c].at[at[AXES[c][0]]], x_sem
        )

    def token(c, d):
        mine = spread[c].at[at[AXES[c][0]]]
        return remote(mine, mine, tok_s.at[c], tok_r.at[c], AXES[c][0], d)

    def forward_token(c, d):
        half = tokens // 2
        theirs = spread[c].at[other(AXES[c][0], SIDE - d), pl.ds(d // 2 * half, half)]
        return remote(theirs, theirs, pass_s.at[c], pass_r.at[c], AXES[c][0], d)

    def two(k, c, d):
        axis = AXES[c][1]
        src, dst = boxes[c].at[other(axis, d)], second(relay[c].at[k], c, at[axis])
        return remote(src, dst, two_s.at[c], two_r.at[k, c], axis, d)

    def piece(c, e, d):
        axis, s = AXES[c][1], other(AXES[c][0], e)
        src = boxes[c].at[other(axis, d), s]
        dst = relay[c].at[0, at[axis], s] if c % 3 == 2 else relay[c].at[0, s, at[axis]]
        return remote(src, dst, two_s.at[c], two_r.at[0, c], axis, d)

    def two_own(k, c):
        p = at[AXES[c][1]]
        return pltpu.make_async_copy(boxes[c].at[p], second(relay[c].at[k], c, p), own.at[0, c])

    def three(k, c, d):
        axis = AXES[c][2]
        src, dst = relay[c].at[k, :, :, other(axis, d)], third(rows[c].at[k], c, at[axis])
        return remote(src, dst, three_s.at[c], three_r.at[k, c], axis, d)

    def three_own(k, c):
        p = at[AXES[c][2]]
        return pltpu.make_async_copy(relay[c].at[k, :, :, p], third(rows[c].at[k], c, p), own.at[1, c])

    def back_three(k, c, d):
        axis = AXES[c][2]
        src, dst = third(rows[c].at[k], c, other(axis, d)), back[c].at[k, at[axis]]
        return remote(src, dst, b3_s.at[c], b3_r.at[k, c], axis, d)

    def back_three_own(k, c):
        p = at[AXES[c][2]]
        return pltpu.make_async_copy(third(rows[c].at[k], c, p), back[c].at[k, p], own.at[2, c])

    def returned(k, c, p):
        return back[c].at[k, :, p] if c % 3 == 2 else back[c].at[k, :, :, p]

    def back_two(k, c, d):
        axis = AXES[c][1]
        src, dst = returned(k, c, other(axis, d)), home[c].at[k, at[axis]]
        return remote(src, dst, b2_s.at[c], b2_r.at[k, c], axis, d)

    def load_home(k, c, d):
        p = other(AXES[c][1], SIDE - d)
        src = returned(k, c, p) if d == 0 else home[c].at[k, p]
        return pltpu.make_async_copy(src, boxes[c].at[p], own.at[3, c])

    def end(c, d):
        axis = AXES[c][0]
        src, dst = spread[c].at[other(axis, d)], sums[c].at[at[axis]]
        return remote(src, dst, end_s.at[c], end_r.at[c], axis, d)

    def weights(n):
        k, cut, s = n // steps, pl.ds(lax.rem(n, steps) * width, width), lax.rem(n, 2)
        return (
            pltpu.make_async_copy(gate_hbm.at[k, :, cut], gate_w.at[s], w_sem.at[s, 0]),
            pltpu.make_async_copy(up_hbm.at[k, :, cut], up_w.at[s], w_sem.at[s, 1]),
            pltpu.make_async_copy(down_hbm.at[k, cut, :], down_w.at[s], w_sem.at[s, 2]),
        )

    def drain(ref, *sems):
        for sem in sems:
            pltpu.make_async_copy(ref, ref, sem).wait()

    def blocks(c, n=SIDE - 1):
        return boxes[c].at[pl.ds(0, n)]


    def place_of_row(k, c):
        r = iota((plane, tokens), 0)
        a1, a2, a3 = AXES[c]
        device = at[a1] * stride[a1] + r // (SIDE * slots) * stride[a2] + r // slots % SIDE * stride[a3]
        return ((2 * device + k) * slots + r % slots).astype(F32)

    def choose_from(k, c, s, place):
        hit = place == metas[c, s, 0:1, :]
        for j in range(1, top):
            hit = hit | (place == metas[c, s, j : j + 1, :])
        mask[c, s] = jnp.where(hit, 1.0, 0.0).astype(BF16)

    def choose(k, c):
        place = place_of_row(k, c)

        def one(s, carry):
            choose_from(k, c, s, place)
            return carry

        lax.fori_loop(0, SIDE, one, 0)

    def weigh(k, c):
        place = place_of_row(k, c)

        def one(s, carry):
            weight = jnp.zeros((plane, tokens), F32)
            for j in range(top):
                gate = metas[c, s, top + j : top + j + 1, :].astype(BF16).astype(F32)
                weight = jnp.where(place == metas[c, s, j : j + 1, :], gate, weight)
            mask[c, s] = weight.astype(BF16)
            return carry

        lax.fori_loop(0, SIDE, one, 0)

    def pack_from(c, s):
        out = dot(mask[c % 3, s], spread[c][s]).astype(BF16)
        boxes[c][:, s] = out.reshape(SIDE, SIDE, slots // GROUP, GROUP, cols[c])

    def pack(c):
        def one(s, carry):
            pack_from(c, s)
            return carry

        lax.fori_loop(0, SIDE, one, 0)

    def combine(k, c):
        span = pl.ds(offset[c], cols[c])

        def one(s, carry):
            got = boxes[c][:, :, s].reshape(plane, cols[c])
            part = lax.dot_general(mask[c % 3, s], got, (((0,), (0,)), ((), ())), preferred_element_type=F32)
            r = pl.ds(pl.multiple_of(s * tokens, tokens), tokens)
            if k == 0:
                acc[r, span] = part
            else:
                part += acc[r, span]
                acc[r, span] = part
                spread[c][s] = part.astype(BF16)
            return carry

        lax.fori_loop(0, SIDE, one, 0)

    def expert(k, errands):
        tile = plane

        def step(f):
            n = k * steps + f
            s = lax.rem(n, 2)
            if n + 1 < 2 * steps:
                for copy in weights(n + 1):
                    copy.start()
            for copy in weights(n):
                copy.wait()

            def body(i, carry):
                r = pl.ds(pl.multiple_of(i * tile, tile), tile)
                if f == 0:
                    for c in PARTS:
                        flat[r, pl.ds(offset[c], cols[c])] = rows[c][k, i].reshape(tile, cols[c])
                z = flat[r, :]
                h = (jax.nn.silu(dot(z, gate_w[s])) * dot(z, up_w[s])).astype(BF16)
                part = dot(h, down_w[s])
                if f == 0:
                    acc[r, :] = part
                elif f < steps - 1:
                    acc[r, :] += part
                else:
                    flat[r, :] = (acc[r, :] + part).astype(BF16)
                    for c in PARTS:
                        out = flat[r, pl.ds(offset[c], cols[c])]
                        rows[c][k, i] = out.reshape(SIDE, SIDE, slots // GROUP, GROUP, cols[c])
                for when, errand in errands:
                    if when // SIDE == f:
                        pl.when(i == when % SIDE)(errand)
                return carry

            lax.fori_loop(0, SIDE, body, 0)

        for f in range(steps):
            with phase(f"expert_{k}{f}"):
                step(f)


    barrier = pltpu.get_barrier_semaphore()
    for axis in range(3):
        for d in OTHERS:
            target = me + (other(axis, d) - at[axis]) * stride[axis]
            pl.semaphore_signal(barrier, inc=1, device_id=(dp, target), device_id_type=MESH)
    arguments = [
        pltpu.make_async_copy(src, dst, arg_sem.at[i])
        for i, (src, dst) in enumerate(((expert_hbm, expert_v), (slot_hbm, slot_v), (score_hbm, score_v)))
    ]
    for copy in arguments:
        copy.start()
    for c in PARTS:
        token_own(c).start()
    for copy in arguments:
        copy.wait()
    slot = slot_v[...]
    meta[0:top, :] = jnp.where(slot < slots, expert_v[...] * slots + slot, -1).astype(F32)
    meta[top:, :] = score_v[...]
    for c in ORDERS:
        metas[c, at[AXES[c][0]]] = meta[...]
    drain(x_hbm, x_sem)
    with phase("barrier"):
        pl.semaphore_wait(barrier, 3 * (SIDE - 1))

    NEAR = (1, SIDE - 1)
    for d in OTHERS:
        for c in ORDERS:
            bell(c, d).start()
    for c in PARTS:
        for d in NEAR:
            token(c, d).start()
    for copy in weights(0):
        copy.start()

    def relay_two(k, c):
        two_own(k, c).wait()
        drain(blocks(c), two_s.at[c], two_r.at[k, c])
        for d in OTHERS:
            three(k, c, d).start()
        three_own(k, c).start()

    def send_boxes(k, c):
        pack(c)
        for d in OTHERS:
            two(k, c, d).start()
        two_own(k, c).start()

    def forward_tokens(c):
        drain(spread[c].at[pl.ds(0, 2)], tok_s.at[c], tok_r.at[c])
        for d in NEAR:
            forward_token(c, d).start()

    def send_pieces(c, e):
        pack_from(c, other(AXES[c][0], e))
        for d in OTHERS:
            piece(c, e, d).start()

    def send_near(c):
        def one(i, carry):
            send_pieces(c, 1 + 2 * i)
            return carry

        lax.fori_loop(0, 2, one, 0)

    for o in ORDERS:
        with phase(f"own_{o}"):
            choose_from(0, o, at[AXES[o][0]], place_of_row(0, o))
            for c in PARTS[o::3]:
                send_pieces(c, 0)
    for c in PARTS:
        with phase(f"pass_{c}"):
            forward_tokens(c)
        if c == 2:
            for o in ORDERS:
                with phase(f"choose_0{o}"):
                    drain(metas.at[o, pl.ds(0, SIDE - 1)], bell_s.at[o], bell_r.at[o])
                    place = place_of_row(0, o)

                    def one(e, carry, o=o, place=place):
                        choose_from(0, o, other(AXES[o][0], e), place)
                        return carry

                    lax.fori_loop(1, SIDE, one, 0)
        if c % 3 == 2:
            for n in range(c - 2, c + 1):
                with phase(f"near_{n}"):
                    send_near(n)
    for c in PARTS:
        with phase(f"spread_wait_{c}"):
            drain(spread[c].at[0], pass_s.at[c], pass_r.at[c])
        with phase(f"pack_0{c}"):
            send_pieces(c, 2)
            two_own(0, c).start()
    with phase("choose_1"):
        for c in ORDERS:
            choose(1, c)
    for c in PARTS:
        with phase(f"relay_two_0{c}"):
            relay_two(0, c)
    for c in PARTS:
        with phase(f"pack_1{c}"):
            send_boxes(1, c)
    with phase("weigh_0"):
        for c in ORDERS:
            weigh(0, c)

    def wait_rows(k):
        for c in PARTS:
            drain(blocks(c), three_s.at[c], three_r.at[k, c])
            three_own(k, c).wait()

    def send_back(k):
        for c in PARTS:
            for d in OTHERS:
                back_three(k, c, d).start()
            back_three_own(k, c).start()

    def relay_back(k, c):
        back_three_own(k, c).wait()
        drain(blocks(c), b3_s.at[c], b3_r.at[k, c])
        for d in OTHERS:
            back_two(k, c, d).start()

    def bring_home(k, c):
        with phase(f"home_{k}{c}"):
            load_home(k, c, 0).start()
            drain(blocks(c), b2_s.at[c], b2_r.at[k, c])
            for d in OTHERS:
                load_home(k, c, d).start()

    def sum_up(k, c):
        with phase(f"load_{k}{c}"):
            drain(blocks(c, SIDE), own.at[3, c])
        with phase(f"combine_{k}{c}"):
            combine(k, c)

    def errands(act, whens):
        out = []
        for c, when in zip(PARTS, whens):

            def errand(c=c):
                with phase(f"{act.__name__}_{c}"):
                    act(c)

            out.append((when, errand))
        return out

    def forward(c):
        relay_two(1, c)

    def forward_back(c):
        relay_back(0, c)

    with phase("wait_rows_0"):
        wait_rows(0)
    expert(0, errands(forward, FIRST))
    send_back(0)
    with phase("wait_rows_1"):
        wait_rows(1)
    expert(1, errands(forward_back, SECOND))
    send_back(1)
    for c in PARTS:
        bring_home(0, c)
        if c % 3 == 2:
            for n in range(c - 2, c + 1):
                sum_up(0, n)
    with phase("weigh_1"):
        for c in ORDERS:
            weigh(1, c)
    for c in PARTS:
        with phase(f"relay_back_1{c}"):
            relay_back(1, c)
    def finish(c):
        sum_up(1, c)
        for d in OTHERS:
            end(c, d).start()

    for c in PARTS:
        bring_home(1, c)
        if c % 3:
            finish(c - 1)
        if c % 3 == 2:
            finish(c)
    for c in PARTS:
        span = pl.ds(offset[c], cols[c])
        axis = AXES[c][0]
        total = acc[pl.ds(pl.multiple_of(at[axis] * tokens, tokens), tokens), span]
        with phase(f"end_{c}"):
            drain(sums[c].at[pl.ds(0, SIDE - 1)], end_s.at[c], end_r.at[c])
        for d in OTHERS:
            total += sums[c][other(axis, d)].astype(F32)
        y_v[:, span] = total.astype(y_v.dtype)
        pltpu.make_async_copy(y_v.at[:, span], y_hbm.at[:, span], y_sem).start()
    with phase("result"):
        drain(y_v, y_sem)


def moe(expert, slot, gate, x, w_gate, w_up, w_down, slots):
    (tokens, depth), inner = x.shape, w_gate.shape[2]
    lanes, more = divmod(depth // 128, len(PARTS))
    cols = tuple(128 * (lanes + (c in WIDE[:more])) for c in PARTS)
    width = min(WIDTH, inner // 2)
    plane = SIDE * SIDE * slots
    box = lambda c, *lead: (*lead, SIDE, SIDE, SIDE, slots // GROUP, GROUP, cols[c])
    hbm = [jax.ShapeDtypeStruct(box(c, 2), BF16) for _ in range(3) for c in PARTS]
    dma = pltpu.SemaphoreType.DMA
    p = len(PARTS)
    out = pl.pallas_call(
        functools.partial(kernel, slots, cols, width),
        in_specs=[pl.BlockSpec(memory_space=pl.ANY)] * 7,
        out_specs=[pl.BlockSpec(memory_space=pl.ANY)] * (1 + len(hbm)),
        out_shape=[jax.ShapeDtypeStruct((tokens, depth), BF16)] + hbm,
        scratch_shapes=[pltpu.VMEM((SIDE, tokens, cols[c]), BF16) for c in PARTS]
        + [pltpu.VMEM(box(c), BF16) for c in PARTS]
        + [pltpu.VMEM(box(c, 2), BF16) for c in PARTS]
        + [pltpu.VMEM((SIDE, tokens, cols[c]), BF16) for c in PARTS]
        + [
            pltpu.VMEM(expert.shape, I32),
            pltpu.VMEM(slot.shape, I32),
            pltpu.VMEM(gate.shape, F32),
            pltpu.VMEM((2 * expert.shape[0], tokens), F32),
            pltpu.VMEM((3, SIDE, 2 * expert.shape[0], tokens), F32),
            pltpu.VMEM((3, SIDE, plane, tokens), BF16),
            pltpu.VMEM((SIDE * plane, depth), BF16),
            pltpu.VMEM((SIDE * plane, depth), F32),
            pltpu.VMEM((2, depth, width), BF16),
            pltpu.VMEM((2, depth, width), BF16),
            pltpu.VMEM((2, width, depth), BF16),
        ]
        + [dma((3,))] * 2
        + [dma((p,))] * 4
        + [dma((p,)), dma((2, p))] * 4
        + [dma((p,))] * 2
        + [dma((4, p)), dma((2, 3)), dma, dma((3,))]
        + [pltpu.VMEM((tokens, depth), BF16), dma],
        compiler_params=pltpu.CompilerParams(
            collective_id=0, has_side_effects=True, vmem_limit_bytes=67043328
        ),
        name="moe",
    )(expert, slot, gate, x, w_gate, w_up, w_down)
    return out[0]


def solution(mesh):
    members = mesh.shape["ep"]

    def step(x, expert, slot, gate, w_gate, w_up, w_down):
        tokens = x.shape[2]
        slots = 5 * tokens * expert.shape[3] // (4 * 2 * members)
        x, expert, slot, gate = x[0, 0], expert[0, 0], slot[0, 0], gate[0, 0]
        return moe(expert.T, slot.T, gate.T, x, w_gate, w_up, w_down, slots)[None, None]

    spread, held = P("dp", "ep"), P("ep")
    return jax.shard_map(
        step,
        mesh=mesh,
        in_specs=(spread, spread, spread, spread, held, held, held),
        out_specs=spread,
        check_vma=False,
    )
```

```python
import contextlib
import functools

import jax
import jax.numpy as jnp
from jax import lax
from jax.experimental import pallas as pl
from jax.experimental.pallas import tpu as pltpu
from jax.sharding import PartitionSpec as P

F32, BF16, I32 = jnp.float32, jnp.bfloat16, jnp.int32
MESH = pl.DeviceIdType.MESH
SIDE = 4
STRIDE = (SIDE * SIDE, SIDE, 1)
AXES = ((0, 1, 2), (1, 2, 0), (2, 0, 1)) * 2
BACK = tuple((c + 2) % 3 for c in range(6))
GROUP = 4
WIDTH = 512
PARTS, ORDERS, OTHERS = range(6), range(3), range(1, SIDE)
FIRST, SECOND = (2, 2, 3, 5, 5, 6), (4, 5, 5, 6, 7, 8)
WIDE = (0, 1, 2, 4, 3, 5)


def phase(name):
    return contextlib.nullcontext()


def iota(shape, dim):
    return lax.broadcasted_iota(I32, shape, dim)


def dot(a, b):
    return jnp.dot(a, b, preferred_element_type=F32)


def kernel(slots, cols, width, expert_hbm, slot_hbm, score_hbm, x_hbm, gate_hbm, up_hbm, down_hbm, y_hbm, *rest):
    rest = list(rest)
    take = lambda n: [rest.pop(0) for _ in range(n)]
    relay, back, home, spread, boxes, rows, sums = (take(len(PARTS)) for _ in range(7))
    expert_v, slot_v, score_v, meta, metas, mask, flat, acc, gate_w, up_w, down_w = take(11)
    bell_s, bell_r, tok_s, tok_r, pass_s, pass_r, two_s, two_r, three_s, three_r = take(10)
    b3_s, b3_r, b2_s, b2_r, end_s, end_r, own, w_sem, x_sem, arg_sem = take(10)
    y_v, y_sem = take(2)

    tokens, depth = x_hbm.shape
    top = expert_v.shape[0]
    inner = gate_hbm.shape[2]
    steps = inner // width
    plane = SIDE * SIDE * slots
    offset = [sum(cols[:c]) for c in PARTS]
    me, dp = lax.axis_index("ep"), lax.axis_index("dp")
    turn = lax.rem(dp, 2)
    chip = (me // STRIDE[0], lax.rem(me // STRIDE[1], SIDE), lax.rem(me, SIDE))
    turned = lambda v: tuple(v[i] + turn * (v[(i + 1) % 3] - v[i]) for i in range(3))
    at, stride = turned(chip), turned(STRIDE)

    def other(axis, d):
        return lax.rem(at[axis] + d, SIDE)

    def remote(src, dst, send, recv, axis, d):
        target = me + (other(axis, d) - at[axis]) * stride[axis]
        return pltpu.make_async_remote_copy(
            src_ref=src, dst_ref=dst, send_sem=send, recv_sem=recv, device_id=(dp, target), device_id_type=MESH
        )


    def third(ref, o, p):
        return (ref.at[:, :, p], ref.at[p], ref.at[:, p])[o % 3]

    def second(ref, o, p):
        return ref.at[p] if o % 3 == 2 else ref.at[:, p]


    def bell(c, d):
        return remote(meta, metas.at[c, at[AXES[c][0]]], bell_s.at[c], bell_r.at[c], AXES[c][0], d)

    def token_own(c):
        return pltpu.make_async_copy(
            x_hbm.at[:, pl.ds(offset[c], cols[c])], spread[c].at[at[AXES[c][0]]], x_sem
        )

    def token(c, d):
        mine = spread[c].at[at[AXES[c][0]]]
        return remote(mine, mine, tok_s.at[c], tok_r.at[c], AXES[c][0], d)

    def forward_token(c, d):
        half = tokens // 2
        theirs = spread[c].at[other(AXES[c][0], SIDE - d), pl.ds(d // 2 * half, half)]
        return remote(theirs, theirs, pass_s.at[c], pass_r.at[c], AXES[c][0], d)

    def two(k, c, d):
        axis = AXES[c][1]
        src, dst = boxes[c].at[other(axis, d)], second(relay[c].at[k], c, at[axis])
        return remote(src, dst, two_s.at[c], two_r.at[k, c], axis, d)

    def piece(c, e, d):
        axis, s = AXES[c][1], other(AXES[c][0], e)
        src = boxes[c].at[other(axis, d), s]
        dst = relay[c].at[0, at[axis], s] if c % 3 == 2 else relay[c].at[0, s, at[axis]]
        return remote(src, dst, two_s.at[c], two_r.at[0, c], axis, d)

    def two_own(k, c):
        p = at[AXES[c][1]]
        return pltpu.make_async_copy(boxes[c].at[p], second(relay[c].at[k], c, p), own.at[0, c])

    def three(k, c, d):
        axis = AXES[c][2]
        src, dst = relay[c].at[k, :, :, other(axis, d)], third(rows[c].at[k], c, at[axis])
        return remote(src, dst, three_s.at[c], three_r.at[k, c], axis, d)

    def three_own(k, c):
        p = at[AXES[c][2]]
        return pltpu.make_async_copy(relay[c].at[k, :, :, p], third(rows[c].at[k], c, p), own.at[1, c])

    def back_three(k, c, d):
        axis = AXES[BACK[c]][2]
        src, dst = third(rows[c].at[k], BACK[c], other(axis, d)), back[c].at[k, at[axis]]
        return remote(src, dst, b3_s.at[c], b3_r.at[k, c], axis, d)

    def back_three_own(k, c):
        p = at[AXES[BACK[c]][2]]
        return pltpu.make_async_copy(third(rows[c].at[k], BACK[c], p), back[c].at[k, p], own.at[2, c])

    def returned(k, c, p):
        return back[c].at[k, :, p] if BACK[c] == 2 else back[c].at[k, :, :, p]

    def back_two(k, c, d):
        axis = AXES[BACK[c]][1]
        src, dst = returned(k, c, other(axis, d)), home[c].at[k, at[axis]]
        return remote(src, dst, b2_s.at[c], b2_r.at[k, c], axis, d)

    def load_home(k, c, d):
        p = other(AXES[BACK[c]][1], SIDE - d)
        src = returned(k, c, p) if d == 0 else home[c].at[k, p]
        return pltpu.make_async_copy(src, boxes[c].at[p], own.at[3, c])

    def end(c, d):
        axis = AXES[BACK[c]][0]
        src, dst = spread[c].at[other(axis, d)], sums[c].at[at[axis]]
        return remote(src, dst, end_s.at[c], end_r.at[c], axis, d)

    def weights(n):
        k, cut, s = n // steps, pl.ds(lax.rem(n, steps) * width, width), lax.rem(n, 2)
        return (
            pltpu.make_async_copy(gate_hbm.at[k, :, cut], gate_w.at[s], w_sem.at[s, 0]),
            pltpu.make_async_copy(up_hbm.at[k, :, cut], up_w.at[s], w_sem.at[s, 1]),
            pltpu.make_async_copy(down_hbm.at[k, cut, :], down_w.at[s], w_sem.at[s, 2]),
        )

    def drain(ref, *sems):
        for sem in sems:
            pltpu.make_async_copy(ref, ref, sem).wait()

    def blocks(c, n=SIDE - 1):
        return boxes[c].at[pl.ds(0, n)]


    def place_of_row(k, c):
        r = iota((plane, tokens), 0)
        a1, a2, a3 = AXES[c]
        device = at[a1] * stride[a1] + r // (SIDE * slots) * stride[a2] + r // slots % SIDE * stride[a3]
        return ((2 * device + k) * slots + r % slots).astype(F32)

    def choose_from(k, c, s, place):
        hit = place == metas[c, s, 0:1, :]
        for j in range(1, top):
            hit = hit | (place == metas[c, s, j : j + 1, :])
        mask[c, s] = jnp.where(hit, 1.0, 0.0).astype(BF16)

    def choose(k, c):
        place = place_of_row(k, c)

        def one(s, carry):
            choose_from(k, c, s, place)
            return carry

        lax.fori_loop(0, SIDE, one, 0)

    def weigh(k, c):
        place = place_of_row(k, c)

        def one(s, carry):
            weight = jnp.zeros((plane, tokens), F32)
            for j in range(top):
                gate = metas[c, s, top + j : top + j + 1, :].astype(BF16).astype(F32)
                weight = jnp.where(place == metas[c, s, j : j + 1, :], gate, weight)
            mask[c, s] = weight.astype(BF16)
            return carry

        lax.fori_loop(0, SIDE, one, 0)

    def pack_from(c, s):
        out = dot(mask[c % 3, s], spread[c][s]).astype(BF16)
        boxes[c][:, s] = out.reshape(SIDE, SIDE, slots // GROUP, GROUP, cols[c])

    def pack(c):
        def one(s, carry):
            pack_from(c, s)
            return carry

        lax.fori_loop(0, SIDE, one, 0)

    def combine(k, c):
        span = pl.ds(offset[c], cols[c])

        def one(s, carry):
            got = boxes[c][:, :, s].reshape(plane, cols[c])
            part = lax.dot_general(mask[BACK[c], s], got, (((0,), (0,)), ((), ())), preferred_element_type=F32)
            r = pl.ds(pl.multiple_of(s * tokens, tokens), tokens)
            if k == 0:
                acc[r, span] = part
            else:
                part += acc[r, span]
                acc[r, span] = part
                spread[c][s] = part.astype(BF16)
            return carry

        lax.fori_loop(0, SIDE, one, 0)

    def expert(k, errands):
        tile = plane

        def step(f):
            n = k * steps + f
            s = lax.rem(n, 2)
            if n + 1 < 2 * steps:
                for copy in weights(n + 1):
                    copy.start()
            for copy in weights(n):
                copy.wait()

            def body(i, carry):
                r = pl.ds(pl.multiple_of(i * tile, tile), tile)
                if f == 0:
                    for c in PARTS:
                        flat[r, pl.ds(offset[c], cols[c])] = rows[c][k, i].reshape(tile, cols[c])
                z = flat[r, :]
                h = (jax.nn.silu(dot(z, gate_w[s])) * dot(z, up_w[s])).astype(BF16)
                part = dot(h, down_w[s])
                if f == 0:
                    acc[r, :] = part
                elif f < steps - 1:
                    acc[r, :] += part
                else:
                    flat[r, :] = (acc[r, :] + part).astype(BF16)
                    for c in PARTS:
                        out = flat[r, pl.ds(offset[c], cols[c])]
                        rows[c][k, i] = out.reshape(SIDE, SIDE, slots // GROUP, GROUP, cols[c])
                for when, errand in errands:
                    if when // SIDE == f:
                        pl.when(i == when % SIDE)(errand)
                return carry

            lax.fori_loop(0, SIDE, body, 0)

        for f in range(steps):
            with phase(f"expert_{k}{f}"):
                step(f)


    barrier = pltpu.get_barrier_semaphore()
    for axis in range(3):
        for d in OTHERS:
            target = me + (other(axis, d) - at[axis]) * stride[axis]
            pl.semaphore_signal(barrier, inc=1, device_id=(dp, target), device_id_type=MESH)
    arguments = [
        pltpu.make_async_copy(src, dst, arg_sem.at[i])
        for i, (src, dst) in enumerate(((expert_hbm, expert_v), (slot_hbm, slot_v), (score_hbm, score_v)))
    ]
    for copy in arguments:
        copy.start()
    for c in PARTS:
        token_own(c).start()
    for copy in arguments:
        copy.wait()
    slot = slot_v[...]
    meta[0:top, :] = jnp.where(slot < slots, expert_v[...] * slots + slot, -1).astype(F32)
    meta[top:, :] = score_v[...]
    for c in ORDERS:
        metas[c, at[AXES[c][0]]] = meta[...]
    drain(x_hbm, x_sem)
    with phase("barrier"):
        pl.semaphore_wait(barrier, 3 * (SIDE - 1))

    NEAR = (1, SIDE - 1)
    for d in OTHERS:
        for c in ORDERS:
            bell(c, d).start()
    for c in PARTS:
        for d in NEAR:
            token(c, d).start()
    for copy in weights(0):
        copy.start()

    def relay_two(k, c):
        two_own(k, c).wait()
        drain(blocks(c), two_s.at[c], two_r.at[k, c])
        for d in OTHERS:
            three(k, c, d).start()
        three_own(k, c).start()

    def send_boxes(k, c):
        pack(c)
        for d in OTHERS:
            two(k, c, d).start()
        two_own(k, c).start()

    def forward_tokens(c):
        drain(spread[c].at[pl.ds(0, 2)], tok_s.at[c], tok_r.at[c])
        for d in NEAR:
            forward_token(c, d).start()

    def send_pieces(c, e):
        pack_from(c, other(AXES[c][0], e))
        for d in OTHERS:
            piece(c, e, d).start()

    def send_near(c):
        def one(i, carry):
            send_pieces(c, 1 + 2 * i)
            return carry

        lax.fori_loop(0, 2, one, 0)

    for o in ORDERS:
        with phase(f"own_{o}"):
            choose_from(0, o, at[AXES[o][0]], place_of_row(0, o))
            for c in PARTS[o::3]:
                send_pieces(c, 0)
    for c in PARTS:
        with phase(f"pass_{c}"):
            forward_tokens(c)
        if c == 2:
            for o in ORDERS:
                with phase(f"choose_0{o}"):
                    drain(metas.at[o, pl.ds(0, SIDE - 1)], bell_s.at[o], bell_r.at[o])
                    place = place_of_row(0, o)

                    def one(e, carry, o=o, place=place):
                        choose_from(0, o, other(AXES[o][0], e), place)
                        return carry

                    lax.fori_loop(1, SIDE, one, 0)
        if c % 3 == 2:
            for n in range(c - 2, c + 1):
                with phase(f"near_{n}"):
                    send_near(n)
    for c in PARTS:
        with phase(f"spread_wait_{c}"):
            drain(spread[c].at[0], pass_s.at[c], pass_r.at[c])
        with phase(f"pack_0{c}"):
            send_pieces(c, 2)
            two_own(0, c).start()
    with phase("choose_1"):
        for c in ORDERS:
            choose(1, c)
    for c in PARTS:
        with phase(f"relay_two_0{c}"):
            relay_two(0, c)
    for c in PARTS:
        with phase(f"pack_1{c}"):
            send_boxes(1, c)
    with phase("weigh_0"):
        for c in ORDERS:
            weigh(0, c)

    def wait_rows(k):
        for c in PARTS:
            drain(blocks(c), three_s.at[c], three_r.at[k, c])
            three_own(k, c).wait()

    def send_back(k):
        for c in PARTS:
            for d in OTHERS:
                back_three(k, c, d).start()
            back_three_own(k, c).start()

    def relay_back(k, c):
        back_three_own(k, c).wait()
        drain(blocks(c), b3_s.at[c], b3_r.at[k, c])
        for d in OTHERS:
            back_two(k, c, d).start()

    def bring_home(k, c):
        with phase(f"home_{k}{c}"):
            load_home(k, c, 0).start()
            drain(blocks(c), b2_s.at[c], b2_r.at[k, c])
            for d in OTHERS:
                load_home(k, c, d).start()

    def sum_up(k, c):
        with phase(f"load_{k}{c}"):
            drain(blocks(c, SIDE), own.at[3, c])
        with phase(f"combine_{k}{c}"):
            combine(k, c)

    def errands(act, whens):
        out = []
        for c, when in zip(PARTS, whens):

            def errand(c=c):
                with phase(f"{act.__name__}_{c}"):
                    act(c)

            out.append((when, errand))
        return out

    def forward(c):
        relay_two(1, c)

    def forward_back(c):
        relay_back(0, c)

    with phase("wait_rows_0"):
        wait_rows(0)
    expert(0, errands(forward, FIRST))
    send_back(0)
    with phase("wait_rows_1"):
        wait_rows(1)
    expert(1, errands(forward_back, SECOND))
    send_back(1)
    for c in PARTS:
        bring_home(0, c)
        if c % 3 == 2:
            for n in range(c - 2, c + 1):
                sum_up(0, n)
    with phase("weigh_1"):
        for c in ORDERS:
            weigh(1, c)
    for c in PARTS:
        with phase(f"relay_back_1{c}"):
            relay_back(1, c)
    def finish(c):
        sum_up(1, c)
        for d in OTHERS:
            end(c, d).start()

    for c in PARTS:
        bring_home(1, c)
        if c % 3:
            finish(c - 1)
        if c % 3 == 2:
            finish(c)
    for c in PARTS:
        span = pl.ds(offset[c], cols[c])
        axis = AXES[BACK[c]][0]
        total = acc[pl.ds(pl.multiple_of(at[axis] * tokens, tokens), tokens), span]
        with phase(f"end_{c}"):
            drain(sums[c].at[pl.ds(0, SIDE - 1)], end_s.at[c], end_r.at[c])
        for d in OTHERS:
            total += sums[c][other(axis, d)].astype(F32)
        y_v[:, span] = total.astype(y_v.dtype)
        pltpu.make_async_copy(y_v.at[:, span], y_hbm.at[:, span], y_sem).start()
    with phase("result"):
        drain(y_v, y_sem)


def moe(expert, slot, gate, x, w_gate, w_up, w_down, slots):
    (tokens, depth), inner = x.shape, w_gate.shape[2]
    lanes, more = divmod(depth // 128, len(PARTS))
    cols = tuple(128 * (lanes + (c in WIDE[:more])) for c in PARTS)
    width = min(WIDTH, inner // 2)
    plane = SIDE * SIDE * slots
    box = lambda c, *lead: (*lead, SIDE, SIDE, SIDE, slots // GROUP, GROUP, cols[c])
    hbm = [jax.ShapeDtypeStruct(box(c, 2), BF16) for _ in range(3) for c in PARTS]
    dma = pltpu.SemaphoreType.DMA
    p = len(PARTS)
    out = pl.pallas_call(
        functools.partial(kernel, slots, cols, width),
        in_specs=[pl.BlockSpec(memory_space=pl.ANY)] * 7,
        out_specs=[pl.BlockSpec(memory_space=pl.ANY)] * (1 + len(hbm)),
        out_shape=[jax.ShapeDtypeStruct((tokens, depth), BF16)] + hbm,
        scratch_shapes=[pltpu.VMEM((SIDE, tokens, cols[c]), BF16) for c in PARTS]
        + [pltpu.VMEM(box(c), BF16) for c in PARTS]
        + [pltpu.VMEM(box(c, 2), BF16) for c in PARTS]
        + [pltpu.VMEM((SIDE, tokens, cols[c]), BF16) for c in PARTS]
        + [
            pltpu.VMEM(expert.shape, I32),
            pltpu.VMEM(slot.shape, I32),
            pltpu.VMEM(gate.shape, F32),
            pltpu.VMEM((2 * expert.shape[0], tokens), F32),
            pltpu.VMEM((3, SIDE, 2 * expert.shape[0], tokens), F32),
            pltpu.VMEM((3, SIDE, plane, tokens), BF16),
            pltpu.VMEM((SIDE * plane, depth), BF16),
            pltpu.VMEM((SIDE * plane, depth), F32),
            pltpu.VMEM((2, depth, width), BF16),
            pltpu.VMEM((2, depth, width), BF16),
            pltpu.VMEM((2, width, depth), BF16),
        ]
        + [dma((3,))] * 2
        + [dma((p,))] * 4
        + [dma((p,)), dma((2, p))] * 4
        + [dma((p,))] * 2
        + [dma((4, p)), dma((2, 3)), dma, dma((3,))]
        + [pltpu.VMEM((tokens, depth), BF16), dma],
        compiler_params=pltpu.CompilerParams(
            collective_id=0, has_side_effects=True, vmem_limit_bytes=67043328
        ),
        name="moe",
    )(expert, slot, gate, x, w_gate, w_up, w_down)
    return out[0]


def solution(mesh):
    members = mesh.shape["ep"]

    def step(x, expert, slot, gate, w_gate, w_up, w_down):
        tokens = x.shape[2]
        slots = 5 * tokens * expert.shape[3] // (4 * 2 * members)
        x, expert, slot, gate = x[0, 0], expert[0, 0], slot[0, 0], gate[0, 0]
        return moe(expert.T, slot.T, gate.T, x, w_gate, w_up, w_down, slots)[None, None]

    spread, held = P("dp", "ep"), P("ep")
    return jax.shard_map(
        step,
        mesh=mesh,
        in_specs=(spread, spread, spread, spread, held, held, held),
        out_specs=spread,
        check_vma=False,
    )
```

```python
import contextlib
import functools

import jax
import jax.numpy as jnp
from jax import lax
from jax.experimental import pallas as pl
from jax.experimental.pallas import tpu as pltpu
from jax.sharding import PartitionSpec as P

F32, BF16, I32 = jnp.float32, jnp.bfloat16, jnp.int32
MESH = pl.DeviceIdType.MESH
SIDE = 4
STRIDE = (SIDE * SIDE, SIDE, 1)
AXES = ((0, 1, 2), (1, 2, 0), (2, 0, 1)) * 3
BACK = tuple((c + 2) % 3 for c in range(9))
GROUP = 4
WIDTH = 512
PARTS, ORDERS, OTHERS = range(9), range(3), range(1, SIDE)
FIRST, SECOND = (2, 2, 3, 4, 4, 5, 6, 6, 6), (4, 4, 5, 5, 6, 6, 7, 8, 8)
WIDE = (0, 1, 2, 3, 4, 5, 7, 6, 8)


def phase(name):
    return contextlib.nullcontext()


def iota(shape, dim):
    return lax.broadcasted_iota(I32, shape, dim)


def dot(a, b):
    return jnp.dot(a, b, preferred_element_type=F32)


def kernel(slots, cols, width, expert_hbm, slot_hbm, score_hbm, x_hbm, gate_hbm, up_hbm, down_hbm, y_hbm, *rest):
    rest = list(rest)
    take = lambda n: [rest.pop(0) for _ in range(n)]
    relay, back, home, spread, boxes, rows, sums = (take(len(PARTS)) for _ in range(7))
    expert_v, slot_v, score_v, meta, metas, mask, flat, acc, gate_w, up_w, down_w = take(11)
    bell_s, bell_r, tok_s, tok_r, pass_s, pass_r, two_s, two_r, three_s, three_r = take(10)
    b3_s, b3_r, b2_s, b2_r, end_s, end_r, own, w_sem, x_sem, arg_sem = take(10)
    y_v, y_sem = take(2)

    tokens, depth = x_hbm.shape
    top = expert_v.shape[0]
    inner = gate_hbm.shape[2]
    steps = inner // width
    plane = SIDE * SIDE * slots
    offset = [sum(cols[:c]) for c in PARTS]
    me, dp = lax.axis_index("ep"), lax.axis_index("dp")
    turn = lax.rem(dp, 2)
    chip = (me // STRIDE[0], lax.rem(me // STRIDE[1], SIDE), lax.rem(me, SIDE))
    turned = lambda v: tuple(v[i] + turn * (v[(i + 1) % 3] - v[i]) for i in range(3))
    at, stride = turned(chip), turned(STRIDE)

    def other(axis, d):
        return lax.rem(at[axis] + d, SIDE)

    def remote(src, dst, send, recv, axis, d):
        target = me + (other(axis, d) - at[axis]) * stride[axis]
        return pltpu.make_async_remote_copy(
            src_ref=src, dst_ref=dst, send_sem=send, recv_sem=recv, device_id=(dp, target), device_id_type=MESH
        )


    def third(ref, o, p):
        return (ref.at[:, :, p], ref.at[p], ref.at[:, p])[o % 3]

    def second(ref, o, p):
        return ref.at[p] if o % 3 == 2 else ref.at[:, p]


    def bell(c, d):
        return remote(meta, metas.at[c, at[AXES[c][0]]], bell_s.at[c], bell_r.at[c], AXES[c][0], d)

    def token_own(c):
        return pltpu.make_async_copy(
            x_hbm.at[:, pl.ds(offset[c], cols[c])], spread[c].at[at[AXES[c][0]]], x_sem
        )

    def token(c, d):
        mine = spread[c].at[at[AXES[c][0]]]
        return remote(mine, mine, tok_s.at[c], tok_r.at[c], AXES[c][0], d)

    def forward_token(c, d):
        half = tokens // 2
        theirs = spread[c].at[other(AXES[c][0], SIDE - d), pl.ds(d // 2 * half, half)]
        return remote(theirs, theirs, pass_s.at[c], pass_r.at[c], AXES[c][0], d)

    def two(k, c, d):
        axis = AXES[c][1]
        src, dst = boxes[c].at[other(axis, d)], second(relay[c].at[k], c, at[axis])
        return remote(src, dst, two_s.at[c], two_r.at[k, c], axis, d)

    def piece(c, e, d):
        axis, s = AXES[c][1], other(AXES[c][0], e)
        src = boxes[c].at[other(axis, d), s]
        dst = relay[c].at[0, at[axis], s] if c % 3 == 2 else relay[c].at[0, s, at[axis]]
        return remote(src, dst, two_s.at[c], two_r.at[0, c], axis, d)

    def two_own(k, c):
        p = at[AXES[c][1]]
        return pltpu.make_async_copy(boxes[c].at[p], second(relay[c].at[k], c, p), own.at[0, c])

    def three(k, c, d):
        axis = AXES[c][2]
        src, dst = relay[c].at[k, :, :, other(axis, d)], third(rows[c].at[k], c, at[axis])
        return remote(src, dst, three_s.at[c], three_r.at[k, c], axis, d)

    def three_own(k, c):
        p = at[AXES[c][2]]
        return pltpu.make_async_copy(relay[c].at[k, :, :, p], third(rows[c].at[k], c, p), own.at[1, c])

    def back_three(k, c, d):
        axis = AXES[BACK[c]][2]
        src, dst = third(rows[c].at[k], BACK[c], other(axis, d)), back[c].at[k, at[axis]]
        return remote(src, dst, b3_s.at[c], b3_r.at[k, c], axis, d)

    def back_three_own(k, c):
        p = at[AXES[BACK[c]][2]]
        return pltpu.make_async_copy(third(rows[c].at[k], BACK[c], p), back[c].at[k, p], own.at[2, c])

    def returned(k, c, p):
        return back[c].at[k, :, p] if BACK[c] == 2 else back[c].at[k, :, :, p]

    def back_two(k, c, d):
        axis = AXES[BACK[c]][1]
        src, dst = returned(k, c, other(axis, d)), home[c].at[k, at[axis]]
        return remote(src, dst, b2_s.at[c], b2_r.at[k, c], axis, d)

    def load_home(k, c, d):
        p = other(AXES[BACK[c]][1], SIDE - d)
        src = returned(k, c, p) if d == 0 else home[c].at[k, p]
        return pltpu.make_async_copy(src, boxes[c].at[p], own.at[3, c])

    def end(c, d):
        axis = AXES[BACK[c]][0]
        src, dst = spread[c].at[other(axis, d)], sums[c].at[at[axis]]
        return remote(src, dst, end_s.at[c], end_r.at[c], axis, d)

    def weights(n):
        k, cut, s = n // steps, pl.ds(lax.rem(n, steps) * width, width), lax.rem(n, 2)
        return (
            pltpu.make_async_copy(gate_hbm.at[k, :, cut], gate_w.at[s], w_sem.at[s, 0]),
            pltpu.make_async_copy(up_hbm.at[k, :, cut], up_w.at[s], w_sem.at[s, 1]),
            pltpu.make_async_copy(down_hbm.at[k, cut, :], down_w.at[s], w_sem.at[s, 2]),
        )

    def drain(ref, *sems):
        for sem in sems:
            pltpu.make_async_copy(ref, ref, sem).wait()

    def blocks(c, n=SIDE - 1):
        return boxes[c].at[pl.ds(0, n)]


    def place_of_row(k, c):
        r = iota((plane, tokens), 0)
        a1, a2, a3 = AXES[c]
        device = at[a1] * stride[a1] + r // (SIDE * slots) * stride[a2] + r // slots % SIDE * stride[a3]
        return ((2 * device + k) * slots + r % slots).astype(F32)

    def choose_from(k, c, s, place):
        hit = place == metas[c, s, 0:1, :]
        for j in range(1, top):
            hit = hit | (place == metas[c, s, j : j + 1, :])
        mask[c, s] = jnp.where(hit, 1.0, 0.0).astype(BF16)

    def choose(k, c):
        place = place_of_row(k, c)

        def one(s, carry):
            choose_from(k, c, s, place)
            return carry

        lax.fori_loop(0, SIDE, one, 0)

    def weigh(k, c):
        place = place_of_row(k, c)

        def one(s, carry):
            weight = jnp.zeros((plane, tokens), F32)
            for j in range(top):
                gate = metas[c, s, top + j : top + j + 1, :].astype(BF16).astype(F32)
                weight = jnp.where(place == metas[c, s, j : j + 1, :], gate, weight)
            mask[c, s] = weight.astype(BF16)
            return carry

        lax.fori_loop(0, SIDE, one, 0)

    def pack_from(c, s):
        out = dot(mask[c % 3, s], spread[c][s]).astype(BF16)
        boxes[c][:, s] = out.reshape(SIDE, SIDE, slots // GROUP, GROUP, cols[c])

    def pack(c):
        def one(s, carry):
            pack_from(c, s)
            return carry

        lax.fori_loop(0, SIDE, one, 0)

    def combine(k, c):
        span = pl.ds(offset[c], cols[c])

        def one(s, carry):
            got = boxes[c][:, :, s].reshape(plane, cols[c])
            part = lax.dot_general(mask[BACK[c], s], got, (((0,), (0,)), ((), ())), preferred_element_type=F32)
            r = pl.ds(pl.multiple_of(s * tokens, tokens), tokens)
            if k == 0:
                acc[r, span] = part
            else:
                part += acc[r, span]
                acc[r, span] = part
                spread[c][s] = part.astype(BF16)
            return carry

        lax.fori_loop(0, SIDE, one, 0)

    def expert(k, errands):
        tile = plane

        def step(f):
            n = k * steps + f
            s = lax.rem(n, 2)
            if n + 1 < 2 * steps:
                for copy in weights(n + 1):
                    copy.start()
            for copy in weights(n):
                copy.wait()

            def body(i, carry):
                r = pl.ds(pl.multiple_of(i * tile, tile), tile)
                if f == 0:
                    for c in PARTS:
                        flat[r, pl.ds(offset[c], cols[c])] = rows[c][k, i].reshape(tile, cols[c])
                z = flat[r, :]
                h = (jax.nn.silu(dot(z, gate_w[s])) * dot(z, up_w[s])).astype(BF16)
                part = dot(h, down_w[s])
                if f == 0:
                    acc[r, :] = part
                elif f < steps - 1:
                    acc[r, :] += part
                else:
                    flat[r, :] = (acc[r, :] + part).astype(BF16)
                    for c in PARTS:
                        out = flat[r, pl.ds(offset[c], cols[c])]
                        rows[c][k, i] = out.reshape(SIDE, SIDE, slots // GROUP, GROUP, cols[c])
                for when, errand in errands:
                    if when // SIDE == f:
                        pl.when(i == when % SIDE)(errand)
                return carry

            lax.fori_loop(0, SIDE, body, 0)

        for f in range(steps):
            with phase(f"expert_{k}{f}"):
                step(f)


    barrier = pltpu.get_barrier_semaphore()
    for axis in range(3):
        for d in OTHERS:
            target = me + (other(axis, d) - at[axis]) * stride[axis]
            pl.semaphore_signal(barrier, inc=1, device_id=(dp, target), device_id_type=MESH)
    arguments = [
        pltpu.make_async_copy(src, dst, arg_sem.at[i])
        for i, (src, dst) in enumerate(((expert_hbm, expert_v), (slot_hbm, slot_v), (score_hbm, score_v)))
    ]
    for copy in arguments:
        copy.start()
    for c in PARTS:
        token_own(c).start()
    for copy in arguments:
        copy.wait()
    slot = slot_v[...]
    meta[0:top, :] = jnp.where(slot < slots, expert_v[...] * slots + slot, -1).astype(F32)
    meta[top:, :] = score_v[...]
    for c in ORDERS:
        metas[c, at[AXES[c][0]]] = meta[...]
    drain(x_hbm, x_sem)
    with phase("barrier"):
        pl.semaphore_wait(barrier, 3 * (SIDE - 1))

    NEAR = (1, SIDE - 1)
    for d in OTHERS:
        for c in ORDERS:
            bell(c, d).start()
    for c in PARTS:
        for d in NEAR:
            token(c, d).start()
    for copy in weights(0):
        copy.start()

    def relay_two(k, c):
        two_own(k, c).wait()
        drain(blocks(c), two_s.at[c], two_r.at[k, c])
        for d in OTHERS:
            three(k, c, d).start()
        three_own(k, c).start()

    def send_boxes(k, c):
        pack(c)
        for d in OTHERS:
            two(k, c, d).start()
        two_own(k, c).start()

    def forward_tokens(c):
        drain(spread[c].at[pl.ds(0, 2)], tok_s.at[c], tok_r.at[c])
        for d in NEAR:
            forward_token(c, d).start()

    def send_pieces(c, e):
        pack_from(c, other(AXES[c][0], e))
        for d in OTHERS:
            piece(c, e, d).start()

    def send_near(c):
        def one(i, carry):
            send_pieces(c, 1 + 2 * i)
            return carry

        lax.fori_loop(0, 2, one, 0)

    for o in ORDERS:
        with phase(f"own_{o}"):
            choose_from(0, o, at[AXES[o][0]], place_of_row(0, o))
            for c in PARTS[o::3]:
                send_pieces(c, 0)
    for c in PARTS:
        with phase(f"pass_{c}"):
            forward_tokens(c)
        if c == 2:
            for o in ORDERS:
                with phase(f"choose_0{o}"):
                    drain(metas.at[o, pl.ds(0, SIDE - 1)], bell_s.at[o], bell_r.at[o])
                    place = place_of_row(0, o)

                    def one(e, carry, o=o, place=place):
                        choose_from(0, o, other(AXES[o][0], e), place)
                        return carry

                    lax.fori_loop(1, SIDE, one, 0)
        if c % 3 == 2:
            for n in range(c - 2, c + 1):
                with phase(f"near_{n}"):
                    send_near(n)
    for c in PARTS:
        with phase(f"spread_wait_{c}"):
            drain(spread[c].at[0], pass_s.at[c], pass_r.at[c])
        with phase(f"pack_0{c}"):
            send_pieces(c, 2)
            two_own(0, c).start()
    with phase("choose_1"):
        for c in ORDERS:
            choose(1, c)
    for c in PARTS:
        with phase(f"relay_two_0{c}"):
            relay_two(0, c)
    for c in PARTS:
        with phase(f"pack_1{c}"):
            send_boxes(1, c)
    with phase("weigh_0"):
        for c in ORDERS:
            weigh(0, c)

    def wait_rows(k):
        for c in PARTS:
            drain(blocks(c), three_s.at[c], three_r.at[k, c])
            three_own(k, c).wait()

    def send_back(k):
        for c in PARTS:
            for d in OTHERS:
                back_three(k, c, d).start()
            back_three_own(k, c).start()

    def relay_back(k, c):
        back_three_own(k, c).wait()
        drain(blocks(c), b3_s.at[c], b3_r.at[k, c])
        for d in OTHERS:
            back_two(k, c, d).start()

    def bring_home(k, c):
        with phase(f"home_{k}{c}"):
            load_home(k, c, 0).start()
            drain(blocks(c), b2_s.at[c], b2_r.at[k, c])
            for d in OTHERS:
                load_home(k, c, d).start()

    def sum_up(k, c):
        with phase(f"load_{k}{c}"):
            drain(blocks(c, SIDE), own.at[3, c])
        with phase(f"combine_{k}{c}"):
            combine(k, c)

    def errands(act, whens):
        out = []
        for c, when in zip(PARTS, whens):

            def errand(c=c):
                with phase(f"{act.__name__}_{c}"):
                    act(c)

            out.append((when, errand))
        return out

    def forward(c):
        relay_two(1, c)

    def forward_back(c):
        relay_back(0, c)

    with phase("wait_rows_0"):
        wait_rows(0)
    expert(0, errands(forward, FIRST))
    send_back(0)
    with phase("wait_rows_1"):
        wait_rows(1)
    expert(1, errands(forward_back, SECOND))
    send_back(1)
    for c in PARTS:
        bring_home(0, c)
        if c % 3 == 2:
            for n in range(c - 2, c + 1):
                sum_up(0, n)
    with phase("weigh_1"):
        for c in ORDERS:
            weigh(1, c)
    for c in PARTS:
        with phase(f"relay_back_1{c}"):
            relay_back(1, c)
    def finish(c):
        sum_up(1, c)
        for d in OTHERS:
            end(c, d).start()

    for c in PARTS:
        bring_home(1, c)
        if c % 3:
            finish(c - 1)
        if c % 3 == 2:
            finish(c)
    for c in PARTS:
        span = pl.ds(offset[c], cols[c])
        axis = AXES[BACK[c]][0]
        total = acc[pl.ds(pl.multiple_of(at[axis] * tokens, tokens), tokens), span]
        with phase(f"end_{c}"):
            drain(sums[c].at[pl.ds(0, SIDE - 1)], end_s.at[c], end_r.at[c])
        for d in OTHERS:
            total += sums[c][other(axis, d)].astype(F32)
        y_v[:, span] = total.astype(y_v.dtype)
        pltpu.make_async_copy(y_v.at[:, span], y_hbm.at[:, span], y_sem).start()
    with phase("result"):
        drain(y_v, y_sem)


def moe(expert, slot, gate, x, w_gate, w_up, w_down, slots):
    (tokens, depth), inner = x.shape, w_gate.shape[2]
    lanes, more = divmod(depth // 128, len(PARTS))
    cols = tuple(128 * (lanes + (c in WIDE[:more])) for c in PARTS)
    width = min(WIDTH, inner // 2)
    plane = SIDE * SIDE * slots
    box = lambda c, *lead: (*lead, SIDE, SIDE, SIDE, slots // GROUP, GROUP, cols[c])
    hbm = [jax.ShapeDtypeStruct(box(c, 2), BF16) for _ in range(3) for c in PARTS]
    dma = pltpu.SemaphoreType.DMA
    p = len(PARTS)
    out = pl.pallas_call(
        functools.partial(kernel, slots, cols, width),
        in_specs=[pl.BlockSpec(memory_space=pl.ANY)] * 7,
        out_specs=[pl.BlockSpec(memory_space=pl.ANY)] * (1 + len(hbm)),
        out_shape=[jax.ShapeDtypeStruct((tokens, depth), BF16)] + hbm,
        scratch_shapes=[pltpu.VMEM((SIDE, tokens, cols[c]), BF16) for c in PARTS]
        + [pltpu.VMEM(box(c), BF16) for c in PARTS]
        + [pltpu.VMEM(box(c, 2), BF16) for c in PARTS]
        + [pltpu.VMEM((SIDE, tokens, cols[c]), BF16) for c in PARTS]
        + [
            pltpu.VMEM(expert.shape, I32),
            pltpu.VMEM(slot.shape, I32),
            pltpu.VMEM(gate.shape, F32),
            pltpu.VMEM((2 * expert.shape[0], tokens), F32),
            pltpu.VMEM((3, SIDE, 2 * expert.shape[0], tokens), F32),
            pltpu.VMEM((3, SIDE, plane, tokens), BF16),
            pltpu.VMEM((SIDE * plane, depth), BF16),
            pltpu.VMEM((SIDE * plane, depth), F32),
            pltpu.VMEM((2, depth, width), BF16),
            pltpu.VMEM((2, depth, width), BF16),
            pltpu.VMEM((2, width, depth), BF16),
        ]
        + [dma((3,))] * 2
        + [dma((p,))] * 4
        + [dma((p,)), dma((2, p))] * 4
        + [dma((p,))] * 2
        + [dma((4, p)), dma((2, 3)), dma, dma((3,))]
        + [pltpu.VMEM((tokens, depth), BF16), dma],
        compiler_params=pltpu.CompilerParams(
            collective_id=0, has_side_effects=True, vmem_limit_bytes=67043328
        ),
        name="moe",
    )(expert, slot, gate, x, w_gate, w_up, w_down)
    return out[0]


def solution(mesh):
    members = mesh.shape["ep"]

    def step(x, expert, slot, gate, w_gate, w_up, w_down):
        tokens = x.shape[2]
        slots = 5 * tokens * expert.shape[3] // (4 * 2 * members)
        x, expert, slot, gate = x[0, 0], expert[0, 0], slot[0, 0], gate[0, 0]
        return moe(expert.T, slot.T, gate.T, x, w_gate, w_up, w_down, slots)[None, None]

    spread, held = P("dp", "ep"), P("ep")
    return jax.shard_map(
        step,
        mesh=mesh,
        in_specs=(spread, spread, spread, spread, held, held, held),
        out_specs=spread,
        check_vma=False,
    )
```
